32 devices in a mesh: ma: 8 (over z, x), freq: 4 (over y, core).
Axes of the slice: x: 2, y: 2, z: 4, core: 2. Of those that a mesh axis runs over, the one named last changes fastest.
Arguments:
- visibilities: bfloat16 [16, 192, 16, 2, 512], P('ma', None, 'freq')
- eigenmodes: bfloat16 [16, 16, 2, 512, 256], P('ma', 'freq'), may hold values from -0.375 to 0.375
- retained: int32 [16], P('ma'), may hold values from 1 to 256
Outputs:
- coefficients: bfloat16 [16, 2, 192, 256], P('ma')
- filtered: bfloat16 [16, 192, 16, 2, 512], P('ma', None, 'freq')
The draws below stay inside these ranges and needn't reach their ends.
All inputs are finite; a program needn't handle non-finite values.
Results may differ from the reference program's by a relative error of at most 0.0049.
Values may be sent and summed in bfloat16 or wider, within the bound.
No kernel may reach another device: no remote copies, remote signals or barrier semaphores. Data moves between devices by JAX's collectives and lax.ppermute only.
A program may use at most 128 MiB of HBM per device.

```python
import jax
import jax.numpy as jnp
from jax import lax

BASE = 512
KMAX = 256
SAMPLES = 192
MODES = 16
FREQS = 16


def draw_visibilities(key, part):
    shape = (MODES, SAMPLES, FREQS, 2, BASE)
    first, second = jax.random.split(key, 2)
    m_scale = 1.0 + 2.0 * jnp.arange(MODES, dtype=jnp.float32) / max(MODES - 1, 1)
    s_scale = jnp.exp(jax.random.uniform(second, (SAMPLES,), jnp.float32) * jnp.log(10.0))
    noise = jax.random.normal(first, shape, jnp.float32)
    values = noise * m_scale[:, None, None, None, None] * s_scale[None, :, None, None, None] / 3.0
    return values.astype(jnp.bfloat16)


def set_ends(result, rng, smallest, top_value):
    longest = result.shape.index(max(result.shape))
    spots = []
    for shift in (0, 1):
        where = [jax.random.randint(jax.random.fold_in(rng, axis), (), 0, length) for axis, length in enumerate(result.shape)]
        where[longest] = (where[longest] + shift) % result.shape[longest]
        spots.append(tuple(where))
    return result.at[spots[0]].set(smallest).at[spots[1]].set(top_value)


def block_scale(stream_key, shape, cuts, smallest, top_value):
    loudness = 1.0
    for dim, shards_of in cuts:
        heights = jax.random.uniform(jax.random.fold_in(jax.random.fold_in(stream_key, 6), dim), (shards_of,), jnp.float32, smallest / len(cuts), top_value / len(cuts))
        loudness = loudness * jnp.repeat(jnp.exp(heights), shape[dim] // shards_of).reshape((-1,) + (1,) * (len(shape) - 1 - dim))
    return loudness


def normal_values(key, shape, scale, most, cuts=(), kind=jnp.bfloat16):
    values = scale * jax.random.normal(key, shape, jnp.float32)
    if cuts:
        values = values * block_scale(key, shape, cuts, -0.22, 0.18)
    return jnp.clip(values, -most, most).astype(kind)


def setup_inputs(seed: int = 0) -> dict:
    key_of = jax.random.split(jax.random.key(seed), 4)
    visibilities = draw_visibilities(jax.random.fold_in(key_of[3], 71), 0)
    eigenmodes = normal_values(key_of[1], (MODES, FREQS, 2, BASE, KMAX), KMAX ** -0.5, 0.375, ((0, 8), (1, 4)))
    retained = set_ends(jax.random.randint(key_of[2], (MODES,), 1, KMAX + 1), jax.random.fold_in(key_of[2], 1), 1, KMAX).astype(jnp.int32)
    return {"visibilities": visibilities, "eigenmodes": eigenmodes, "retained": retained}


def reference(visibilities, eigenmodes, retained):
    modes_all, samples, freqs, _, base = visibilities.shape
    kmax = eigenmodes.shape[-1]
    width = freqs * 2 * base

    def project(item):
        vis, vecs = item
        flat = vis.reshape(samples, width)
        swapped = jnp.stack([vis[:, :, 1, :], -vis[:, :, 0, :]], axis=2).reshape(samples, width)
        matrix = vecs.reshape(width, kmax)
        return (jnp.dot(flat, matrix, preferred_element_type=jnp.float32), jnp.dot(swapped, matrix, preferred_element_type=jnp.float32))
    proj_re, proj_im = lax.map(project, (visibilities, eigenmodes))
    keep = (jnp.arange(kmax, dtype=jnp.int32)[None, :] < retained[:, None]).astype(jnp.float32)
    power = lax.optimization_barrier(jnp.sum(keep[:, None, :] * (proj_re * proj_re + proj_im * proj_im), axis=(0, 1)))
    count = jnp.float32(samples) * lax.optimization_barrier(jnp.sum(keep, axis=0))
    scale = 1.0 / jnp.sqrt(power / jnp.maximum(count, 1.0) + 1e-06)
    gain = keep * scale[None, :]
    coef_re = (proj_re * gain[:, None, :]).astype(jnp.bfloat16)
    coef_im = (proj_im * gain[:, None, :]).astype(jnp.bfloat16)

    def back(item):
        cre, cim, vecs = item
        matrix = vecs.reshape(width, kmax)
        first = jnp.dot(cre, matrix.T, preferred_element_type=jnp.float32).reshape(samples, freqs, 2, base)
        second = jnp.dot(cim, matrix.T, preferred_element_type=jnp.float32).reshape(samples, freqs, 2, base)
        out_re = first[:, :, 0, :] - second[:, :, 1, :]
        out_im = second[:, :, 0, :] + first[:, :, 1, :]
        return jnp.stack([out_re, out_im], axis=2).astype(jnp.bfloat16)
    filtered = lax.map(back, (coef_re, coef_im, eigenmodes))
    coefficients = jnp.stack([coef_re, coef_im], axis=1)
    return (coefficients, filtered)
```

```python
import functools

import jax
import jax.numpy as jnp
from jax import lax
from jax.experimental import pallas as pl
from jax.experimental.pallas import tpu as pltpu
from jax.sharding import PartitionSpec as P

F32 = jnp.float32
BF16 = jnp.bfloat16


def times_i(x):
    up = pltpu.roll(x, x.shape[0] - 1, 0)
    down = pltpu.roll(x, 1, 0)
    even = (lax.broadcasted_iota(jnp.int32, x.shape, 0) & 1) == 0
    return jnp.where(even, -up, down)


def project_kernel(mode_ref, v_ref, e_ref, out_ref, acc):
    f = pl.program_id(0)
    samples, base = v_ref.shape[1], v_ref.shape[-1]
    rows = v_ref[0, :, 0].reshape(2 * samples, base)
    by_re = jnp.dot(rows, e_ref[0, 0, 0], preferred_element_type=F32)
    by_im = jnp.dot(rows, e_ref[0, 0, 1], preferred_element_type=F32)

    @pl.when(f == 0)
    def _():
        acc[0] = by_re
        acc[1] = by_im

    @pl.when(f > 0)
    def _():
        acc[0] += by_re
        acc[1] += by_im

    @pl.when(f == pl.num_programs(0) - 1)
    def _():
        out_ref[...] = (acc[0] - times_i(acc[1])).astype(out_ref.dtype)


def project(mode, v, e, dtype):
    _, samples, freqs, _, base = v.shape
    kmax = e.shape[-1]
    return pl.pallas_call(
        project_kernel,
        grid_spec=pltpu.PrefetchScalarGridSpec(
            num_scalar_prefetch=1,
            grid=(freqs,),
            in_specs=[
                pl.BlockSpec((1, samples, 1, 2, base), lambda f, mode: (mode[0], 0, f, 0, 0)),
                pl.BlockSpec((1, 1, 2, base, kmax), lambda f, mode: (mode[0], f, 0, 0, 0)),
            ],
            out_specs=pl.BlockSpec((2 * samples, kmax), lambda f, mode: (0, 0)),
            scratch_shapes=[pltpu.VMEM((2, 2 * samples, kmax), F32)],
        ),
        out_shape=jax.ShapeDtypeStruct((2 * samples, kmax), dtype),
        name="project",
        cost_estimate=pl.CostEstimate(
            flops=8 * samples * freqs * base * kmax,
            bytes_accessed=4 * (samples * freqs * base + freqs * base * kmax),
            transcendentals=0,
        ),
    )(mode, v, e)


def power_kernel(mode_ref, retained_ref, mine_ref, theirs_ref, total_ref, stats_ref):
    total = mine_ref[...].astype(F32) + theirs_ref[...].astype(F32)
    total_ref[...] = total.astype(total_ref.dtype)
    kmax = total.shape[1]
    keep = lax.broadcasted_iota(jnp.int32, (1, kmax), 1) < retained_ref[mode_ref[0]]
    keep = keep.astype(F32)
    power = keep * jnp.sum(total * total, axis=0, keepdims=True)
    stats = jnp.concatenate([power, keep], axis=0)
    stats_ref[...] = jnp.broadcast_to(stats[None], stats_ref.shape)


def power_of(mode, retained, mine, theirs, peers):
    rows, kmax = mine.shape
    return pl.pallas_call(
        power_kernel,
        grid_spec=pltpu.PrefetchScalarGridSpec(
            num_scalar_prefetch=2,
            grid=(1,),
            in_specs=[pl.BlockSpec((rows, kmax), lambda i, a, b: (0, 0))] * 2,
            out_specs=[
                pl.BlockSpec((rows, kmax), lambda i, a, b: (0, 0)),
                pl.BlockSpec((peers, 2, kmax), lambda i, a, b: (0, 0, 0)),
            ],
        ),
        out_shape=[
            jax.ShapeDtypeStruct((rows, kmax), BF16),
            jax.ShapeDtypeStruct((peers, 2, kmax), F32),
        ],
        name="power",
    )(mode, retained, mine, theirs)


def back_kernel(first_ref, retained_ref, copies, stats_ref, mine_ref, other_ref, e_ref, coef_ref, out_ref, pair, flat):
    m, f = pl.program_id(0), pl.program_id(1)
    rows, kmax = mine_ref.shape
    samples = rows // 2

    def prepare(proj_ref):
        stats = jnp.sum(stats_ref[...], axis=0) * F32(1.0 / copies)
        power, count = stats[0:1], F32(samples) * stats[1:2]
        scale = 1.0 / jnp.sqrt(power / jnp.maximum(count, 1.0) + 1e-06)
        keep = lax.broadcasted_iota(jnp.int32, (1, kmax), 1) < retained_ref[m]
        gain = keep.astype(F32) * scale
        coef = proj_ref[...].astype(F32) * gain
        lanes = flat.shape[2]
        for i in range(flat.shape[0]):
            flat[i] = coef[:, i * lanes : (i + 1) * lanes]
            for part in range(2):
                every = flat[i, pl.ds(part, samples, stride=2), :]
                coef_ref[0, part, :, i * lanes : (i + 1) * lanes] = every.astype(BF16)
        pair[:, :kmax] = coef.astype(BF16)
        pair[:, kmax:] = times_i(coef).astype(BF16)

    @pl.when((f == 0) & (m == first_ref[0]))
    def _():
        prepare(mine_ref)

    @pl.when((f == 0) & (m != first_ref[0]))
    def _():
        prepare(other_ref)

    contract = (((1,), (1,)), ((), ()))
    out = lax.dot_general(pair[:, :kmax], e_ref[0, 0, 0], contract, preferred_element_type=F32)
    out += lax.dot_general(pair[:, kmax:], e_ref[0, 0, 1], contract, preferred_element_type=F32)
    out_ref[0, :, 0] = out.astype(BF16).reshape(samples, 2, out.shape[1])


def back(first, retained, copies, stats, mine, other, e):
    rows, kmax = mine.shape
    modes, freqs, _, base, _ = e.shape
    samples = rows // 2
    whole = lambda *shape: pl.BlockSpec(shape, lambda m, f, a, b: (0,) * len(shape))
    return pl.pallas_call(
        lambda first_ref, retained_ref, *refs: back_kernel(first_ref, retained_ref, copies, *refs),
        grid_spec=pltpu.PrefetchScalarGridSpec(
            num_scalar_prefetch=2,
            grid=(modes, freqs),
            in_specs=[
                whole(*stats.shape),
                whole(rows, kmax),
                whole(rows, kmax),
                pl.BlockSpec((1, 1, 2, base, kmax), lambda m, f, a, b: (m, f, 0, 0, 0)),
            ],
            out_specs=[
                pl.BlockSpec((1, 2, samples, kmax), lambda m, f, a, b: (m, 0, 0, 0)),
                pl.BlockSpec((1, samples, 1, 2, base), lambda m, f, a, b: (m, 0, f, 0, 0)),
            ],
            scratch_shapes=[pltpu.VMEM((rows, 2 * kmax), BF16), pltpu.VMEM((kmax // 128, rows, 128), F32)],
        ),
        out_shape=[
            jax.ShapeDtypeStruct((modes, 2, samples, kmax), BF16),
            jax.ShapeDtypeStruct((modes, samples, freqs, 2, base), BF16),
        ],
        name="back",
    )(first, retained, stats, mine, other, e)


def per_device(visibilities, eigenmodes, retained):
    freq_size, ma_size = lax.axis_size("freq"), lax.axis_size("ma")
    place = lax.axis_index("freq")

    def swap(x, bit):
        return lax.ppermute(x, "freq", [(i, i ^ bit) for i in range(freq_size)])

    kept = (place & 1).astype(jnp.int32).reshape(1)
    given = 1 - kept
    received = swap(project(given, visibilities, eigenmodes, BF16), 1)
    total = (project(kept, visibilities, eigenmodes, F32) + received.astype(F32)).astype(BF16)
    bit = 2
    while 2 * bit < freq_size:
        total = (total.astype(F32) + swap(total, bit).astype(F32)).astype(BF16)
        bit *= 2
    theirs = swap(total, bit)
    peers = ma_size * freq_size
    mine, stats = power_of(kept, retained, total, theirs, peers)
    other = swap(mine, 1)
    stats = lax.all_to_all(stats, ("ma", "freq"), 0, 0, tiled=True)
    coefficients, filtered = back(kept, retained, freq_size // 2, stats, mine, other, eigenmodes)
    return coefficients, filtered


def solution(mesh):
    return jax.shard_map(
        per_device,
        mesh=mesh,
        in_specs=(P("ma", None, "freq", None, None), P("ma", "freq", None, None, None), P("ma")),
        out_specs=(P("ma", None, None, None), P("ma", None, "freq", None, None)),
        check_vma=False,
    )
```

```python
import functools

import jax
import jax.numpy as jnp
from jax import lax
from jax.experimental import pallas as pl
from jax.experimental.pallas import tpu as pltpu
from jax.sharding import PartitionSpec as P

F32 = jnp.float32
BF16 = jnp.bfloat16
VMEM = pl.BlockSpec(memory_space=pltpu.VMEM)
SMEM = pl.BlockSpec(memory_space=pltpu.SMEM)
HBM = pl.BlockSpec(memory_space=pltpu.HBM)
MIB = 1 << 20


def limit(vmem):
    return pltpu.CompilerParams(vmem_limit_bytes=vmem)


def times_i(x):
    up = pltpu.roll(x, x.shape[0] - 1, 0)
    down = pltpu.roll(x, 1, 0)
    even = (lax.broadcasted_iota(jnp.int32, x.shape, 0) & 1) == 0
    return jnp.where(even, -up, down)


def project_kernel(first_ref, v_hbm, e_hbm, given_ref, kept_ref, e_ref, v_buf, acc, v_sem, e_sem):
    modes, freqs, samples, _, base = v_buf.shape
    rows = 2 * samples
    half = modes // 2
    mode = [lax.rem(first_ref[0] + j, modes) for j in range(modes)]
    copies = []
    for j in range(modes):
        for f in range(freqs):
            e_copy = pltpu.make_async_copy(e_hbm.at[mode[j], f], e_ref.at[mode[j], f], e_sem.at[j, f])
            v_copy = pltpu.make_async_copy(v_hbm.at[mode[j], :, f], v_buf.at[j, f], v_sem.at[j, f])
            e_copy.start()
            v_copy.start()
            copies.append((e_copy, v_copy))
    for j in range(modes):
        for f in range(freqs):
            for copy in copies[j * freqs + f]:
                copy.wait()
            x = v_buf[j, f].reshape(rows, base)
            by_re = jnp.dot(x, e_ref[mode[j], f, 0], preferred_element_type=F32)
            by_im = jnp.dot(x, e_ref[mode[j], f, 1], preferred_element_type=F32)
            if f > 0:
                by_re += acc[0]
                by_im += acc[1]
            if f < freqs - 1:
                acc[0] = by_re
                acc[1] = by_im
            else:
                out_ref = given_ref if j < half else kept_ref
                out = by_re - times_i(by_im)
                out_ref[pl.ds(j % half * rows, rows), :] = out.astype(out_ref.dtype)


def project(first, v, e):
    modes, samples, freqs, _, base = v.shape
    kmax = e.shape[-1]
    rows = modes // 2 * 2 * samples
    return pl.pallas_call(
        project_kernel,
        in_specs=[SMEM, HBM, HBM],
        out_specs=[VMEM, VMEM, VMEM],
        out_shape=[
            jax.ShapeDtypeStruct((rows, kmax), BF16),
            jax.ShapeDtypeStruct((rows, kmax), F32),
            jax.ShapeDtypeStruct(e.shape, e.dtype),
        ],
        scratch_shapes=[
            pltpu.VMEM((modes, freqs, samples, 2, base), v.dtype),
            pltpu.VMEM((2, 2 * samples, kmax), F32),
            pltpu.SemaphoreType.DMA((modes, freqs)),
            pltpu.SemaphoreType.DMA((modes, freqs)),
        ],
        name="project",
        compiler_params=limit(MIB * 16),
    )(first, pltpu.with_memory_space_constraint(v, pltpu.HBM), pltpu.with_memory_space_constraint(e, pltpu.HBM))


def power_kernel(first_ref, retained_ref, mine_ref, theirs_ref, total_ref, stats_ref):
    modes = retained_ref.shape[0]
    half = modes // 2
    kmax = mine_ref.shape[1]
    rows = mine_ref.shape[0] // half
    stats = jnp.zeros((2, kmax), F32)
    for j in range(half):
        at = pl.ds(j * rows, rows)
        total = mine_ref[at, :].astype(F32) + theirs_ref[at, :].astype(F32)
        total_ref[at, :] = total.astype(total_ref.dtype)
        keep = lax.broadcasted_iota(jnp.int32, (1, kmax), 1) < retained_ref[lax.rem(first_ref[0] + j, modes)]
        keep = keep.astype(F32)
        power = keep * jnp.sum(total * total, axis=0, keepdims=True)
        stats += jnp.concatenate([power, keep], axis=0)
    stats_ref[...] = jnp.broadcast_to(stats[None], stats_ref.shape)


def power_of(first, retained, mine, theirs, peers):
    rows, kmax = mine.shape
    return pl.pallas_call(
        power_kernel,
        in_specs=[SMEM, SMEM, VMEM, VMEM],
        out_specs=[VMEM, VMEM],
        out_shape=[
            jax.ShapeDtypeStruct((rows, kmax), BF16),
            jax.ShapeDtypeStruct((peers, 2, kmax), F32),
        ],
        name="power",
        compiler_params=limit(MIB * 4),
    )(first, retained, mine, theirs)


def back_kernel(
    copies, first_ref, retained_ref, stats_ref, mine_ref, other_ref, e_ref, coef_hbm, out_hbm, pair, flat, coef_buf, out_buf, coef_sem, out_sem
):
    modes, freqs, samples, _, base = out_buf.shape
    kmax = mine_ref.shape[1]
    rows = 2 * samples
    half = modes // 2
    lanes = flat.shape[2]
    stats = jnp.sum(stats_ref[...], axis=0) * F32(1.0 / copies)
    power, count = stats[0:1], F32(samples) * stats[1:2]
    scale = 1.0 / jnp.sqrt(power / jnp.maximum(count, 1.0) + 1e-06)
    contract = (((1,), (1,)), ((), ()))
    pending = []
    for j in range(modes):
        mode = lax.rem(first_ref[0] + j, modes)
        proj_ref = mine_ref if j < half else other_ref
        keep = lax.broadcasted_iota(jnp.int32, (1, kmax), 1) < retained_ref[mode]
        gain = keep.astype(F32) * scale
        coef = proj_ref[pl.ds(j % half * rows, rows), :].astype(F32) * gain
        pair[:, :kmax] = coef.astype(BF16)
        pair[:, kmax:] = times_i(coef).astype(BF16)
        for i in range(kmax // lanes):
            flat[i] = coef[:, i * lanes : (i + 1) * lanes]
            for part in range(2):
                every = flat[i, pl.ds(part, samples, stride=2), :]
                coef_buf[j, part, :, i * lanes : (i + 1) * lanes] = every.astype(BF16)
        copy = pltpu.make_async_copy(coef_buf.at[j], coef_hbm.at[mode], coef_sem.at[j])
        copy.start()
        pending.append(copy)
        for f in range(freqs):
            out = lax.dot_general(pair[:, :kmax], e_ref[mode, f, 0], contract, preferred_element_type=F32)
            out += lax.dot_general(pair[:, kmax:], e_ref[mode, f, 1], contract, preferred_element_type=F32)
            out_buf[j, f] = out.astype(BF16).reshape(samples, 2, base)
            copy = pltpu.make_async_copy(out_buf.at[j, f], out_hbm.at[mode, :, f], out_sem.at[j, f])
            copy.start()
            pending.append(copy)
    for copy in pending:
        copy.wait()


def back(first, retained, copies, stats, mine, other, e):
    kmax = mine.shape[1]
    modes, freqs, _, base, _ = e.shape
    samples = mine.shape[0] // modes
    return pl.pallas_call(
        functools.partial(back_kernel, copies),
        in_specs=[SMEM, SMEM, VMEM, VMEM, VMEM, VMEM],
        out_specs=[HBM, HBM],
        out_shape=[
            jax.ShapeDtypeStruct((modes, 2, samples, kmax), BF16),
            jax.ShapeDtypeStruct((modes, samples, freqs, 2, base), BF16),
        ],
        scratch_shapes=[
            pltpu.VMEM((2 * samples, 2 * kmax), BF16),
            pltpu.VMEM((kmax // 128, 2 * samples, 128), F32),
            pltpu.VMEM((modes, 2, samples, kmax), BF16),
            pltpu.VMEM((modes, freqs, samples, 2, base), BF16),
            pltpu.SemaphoreType.DMA((modes,)),
            pltpu.SemaphoreType.DMA((modes, freqs)),
        ],
        name="back",
        compiler_params=limit(MIB * 16),
    )(first, retained, stats, mine, other, e)


def per_device(visibilities, eigenmodes, retained):
    freq_size, ma_size = lax.axis_size("freq"), lax.axis_size("ma")
    half = visibilities.shape[0] // 2
    side = (lax.axis_index("freq") & 1).astype(jnp.int32).reshape(1)

    def swap(x, bit):
        return lax.ppermute(x, "freq", [(i, i ^ bit) for i in range(freq_size)])

    first_kept, first_given = side * half, (1 - side) * half
    given, kept, e_vmem = project(first_given, visibilities, eigenmodes)
    total = (kept + swap(given, 1).astype(F32)).astype(BF16)
    bit = 2
    while 2 * bit < freq_size:
        total = (total.astype(F32) + swap(total, bit).astype(F32)).astype(BF16)
        bit *= 2
    mine, stats = power_of(first_kept, retained, total, swap(total, bit), ma_size * freq_size)
    other = swap(mine, 1)
    stats = lax.all_to_all(stats, ("ma", "freq"), 0, 0, tiled=True)
    coefficients, filtered = back(first_kept, retained, freq_size // 2, stats, mine, other, e_vmem)
    return coefficients, filtered


def solution(mesh):
    return jax.shard_map(
        per_device,
        mesh=mesh,
        in_specs=(P("ma", None, "freq", None, None), P("ma", "freq", None, None, None), P("ma")),
        out_specs=(P("ma", None, None, None), P("ma", None, "freq", None, None)),
        check_vma=False,
    )
```

```python
import functools

import jax
import jax.numpy as jnp
from jax import lax
from jax.experimental import pallas as pl
from jax.experimental.pallas import tpu as pltpu
from jax.sharding import PartitionSpec as P

F32 = jnp.float32
BF16 = jnp.bfloat16
VMEM = pl.BlockSpec(memory_space=pltpu.VMEM)
SMEM = pl.BlockSpec(memory_space=pltpu.SMEM)
HBM = pl.BlockSpec(memory_space=pltpu.HBM)
MIB = 1 << 20


def limit(vmem):
    return pltpu.CompilerParams(vmem_limit_bytes=vmem)


def cost(flops, *arrays):
    moved = sum(a.size * a.dtype.itemsize for a in arrays)
    return pl.CostEstimate(flops=flops, bytes_accessed=moved, transcendentals=0)


def times_i(x):
    up = pltpu.roll(x, x.shape[0] - 1, 0)
    down = pltpu.roll(x, 1, 0)
    even = (lax.broadcasted_iota(jnp.int32, x.shape, 0) & 1) == 0
    return jnp.where(even, -up, down)


def project_kernel(place_ref, v_hbm, e_hbm, given_ref, kept_ref, e_kept, e_given, v_buf, acc, v_sem, e_sem):
    modes, freqs, samples, _, base = v_buf.shape
    rows = 2 * samples
    half = modes // 2
    first, later = (1 - place_ref[0]) * half, place_ref[1]
    mode = [lax.rem(first + j, modes) for j in range(modes)]
    e_of = [e_given.at[j] for j in range(half)] + [e_kept.at[j] for j in range(half)]
    copies = []
    for j in range(modes):
        for f in range(freqs):
            e_copy = pltpu.make_async_copy(e_hbm.at[mode[j], f], e_of[j].at[f], e_sem.at[j, f])
            v_copy = pltpu.make_async_copy(v_hbm.at[mode[j], :, f], v_buf.at[j, f], v_sem.at[j, f])
            e_copy.start()
            v_copy.start()
            copies.append((e_copy, v_copy))
    for j in range(modes):
        for f in range(freqs):
            for copy in copies[j * freqs + f]:
                copy.wait()
            x = v_buf[j, f].reshape(rows, base)
            by_re = jnp.dot(x, e_of[j][f, 0], preferred_element_type=F32)
            by_im = jnp.dot(x, e_of[j][f, 1], preferred_element_type=F32)
            if f > 0:
                by_re += acc[0]
                by_im += acc[1]
            if f < freqs - 1:
                acc[0] = by_re
                acc[1] = by_im
            else:
                out_ref = given_ref if j < half else kept_ref
                out = (by_re - times_i(by_im)).astype(out_ref.dtype)
                out_ref[1 - later, j % half] = out[:samples]
                out_ref[later, j % half] = out[samples:]


def project(place, v, e):
    modes, samples, freqs, _, base = v.shape
    kmax = e.shape[-1]
    shape = (2, modes // 2, samples, kmax)
    return pl.pallas_call(
        project_kernel,
        in_specs=[SMEM, HBM, HBM],
        out_specs=[VMEM, VMEM, VMEM],
        out_shape=[
            jax.ShapeDtypeStruct(shape, BF16),
            jax.ShapeDtypeStruct(shape, F32),
            jax.ShapeDtypeStruct((modes // 2,) + e.shape[1:], e.dtype),
        ],
        scratch_shapes=[
            pltpu.VMEM((modes // 2,) + e.shape[1:], e.dtype),
            pltpu.VMEM((modes, freqs, samples, 2, base), v.dtype),
            pltpu.VMEM((2, 2 * samples, kmax), F32),
            pltpu.SemaphoreType.DMA((modes, freqs)),
            pltpu.SemaphoreType.DMA((modes, freqs)),
        ],
        name="project",
        cost_estimate=cost(8 * modes * samples * freqs * base * kmax, v, e),
        compiler_params=limit(MIB * 16),
    )(place, pltpu.with_memory_space_constraint(v, pltpu.HBM), pltpu.with_memory_space_constraint(e, pltpu.HBM))


def power_kernel(place_ref, retained_ref, mine_ref, theirs_ref, total_ref, stats_ref):
    half, _, kmax = mine_ref.shape
    power, kept = jnp.zeros((1, kmax), F32), jnp.zeros((1, kmax), F32)
    for j in range(half):
        total = mine_ref[j] + theirs_ref[j].astype(F32)
        total_ref[j] = total.astype(total_ref.dtype)
        keep = lax.broadcasted_iota(jnp.int32, (1, kmax), 1) < retained_ref[place_ref[0] * half + j]
        keep = keep.astype(F32)
        power += keep * jnp.sum(total * total, axis=0, keepdims=True)
        kept += keep
    stats = jnp.concatenate([power, kept], axis=0)
    stats_ref[...] = jnp.broadcast_to(stats[None], stats_ref.shape)


def power_of(place, retained, mine, theirs, peers):
    kmax = mine.shape[-1]
    return pl.pallas_call(
        power_kernel,
        in_specs=[SMEM, SMEM, VMEM, VMEM],
        out_specs=[VMEM, VMEM],
        out_shape=[
            jax.ShapeDtypeStruct(mine.shape, BF16),
            jax.ShapeDtypeStruct((peers, 2, kmax), F32),
        ],
        name="power",
        compiler_params=limit(MIB * 4),
    )(place, retained, mine, theirs)


def back_kernel(
    freq_size, place_ref, retained_ref, stats_ref, q0_ref, q1_ref, q2_ref, q3_ref, e_kept, e_hbm, coef_hbm, out_hbm, e_other, pair, flat, coef_buf, out_buf, e_sem, coef_sem, out_sem
):
    modes, freqs, samples, _, base = out_buf.shape
    kmax = q0_ref.shape[-1]
    half = modes // 2
    lanes = flat.shape[2]
    mode = [lax.rem(place_ref[0] * half + j, modes) for j in range(modes)]
    fetches = []
    for j in range(half):
        for f in range(freqs):
            fetch = pltpu.make_async_copy(e_hbm.at[mode[half + j], f], e_other.at[j, f], e_sem.at[j, f])
            fetch.start()
            fetches.append(fetch)
    stats = jnp.sum(stats_ref[...], axis=0)
    power = stats[0:1] * F32(4 / freq_size)
    count = F32(samples) * stats[1:2] * F32(2 / freq_size)
    scale = 1.0 / jnp.sqrt(power / jnp.maximum(count, 1.0) + 1e-06)
    contract = (((1,), (1,)), ((), ()))
    pending = []
    for j in range(modes):
        keep = lax.broadcasted_iota(jnp.int32, (1, kmax), 1) < retained_ref[mode[j]]
        gain = keep.astype(F32) * scale
        parts = (q0_ref, q2_ref) if j < half else (q1_ref, q3_ref)
        for part, side in zip(parts, (place_ref[1], 1 - place_ref[1])):
            coef = part[j % half].astype(F32) * gain
            at = pl.ds(pl.multiple_of(side * samples, samples), samples)
            pair[at, :kmax] = coef.astype(BF16)
            pair[at, kmax:] = times_i(coef).astype(BF16)
            for i in range(kmax // lanes):
                flat[i, at, :] = coef[:, i * lanes : (i + 1) * lanes]
        for i in range(kmax // lanes):
            for c in range(2):
                every = flat[i, pl.ds(c, samples, stride=2), :]
                coef_buf[j, c, :, i * lanes : (i + 1) * lanes] = every.astype(BF16)
        copy = pltpu.make_async_copy(coef_buf.at[j], coef_hbm.at[mode[j]], coef_sem.at[j])
        copy.start()
        pending.append(copy)
        for f in range(freqs):
            if j >= half:
                fetches[(j - half) * freqs + f].wait()
            e_ref = e_kept.at[j, f] if j < half else e_other.at[j - half, f]
            out = lax.dot_general(pair[:, :kmax], e_ref[0], contract, preferred_element_type=F32)
            out += lax.dot_general(pair[:, kmax:], e_ref[1], contract, preferred_element_type=F32)
            out_buf[j, f] = out.astype(BF16).reshape(samples, 2, base)
            copy = pltpu.make_async_copy(out_buf.at[j, f], out_hbm.at[mode[j], :, f], out_sem.at[j, f])
            copy.start()
            pending.append(copy)
    for copy in pending:
        copy.wait()


def back(place, retained, freq_size, stats, quarters, e_kept, e):
    modes, freqs, _, base, kmax = e.shape
    samples = quarters[0].shape[1]
    return pl.pallas_call(
        functools.partial(back_kernel, freq_size),
        in_specs=[SMEM, SMEM] + [VMEM] * 6 + [HBM],
        out_specs=[HBM, HBM],
        out_shape=[
            jax.ShapeDtypeStruct((modes, 2, samples, kmax), BF16),
            jax.ShapeDtypeStruct((modes, samples, freqs, 2, base), BF16),
        ],
        scratch_shapes=[
            pltpu.VMEM(e_kept.shape, e.dtype),
            pltpu.VMEM((2 * samples, 2 * kmax), BF16),
            pltpu.VMEM((kmax // 128, 2 * samples, 128), F32),
            pltpu.VMEM((modes, 2, samples, kmax), BF16),
            pltpu.VMEM((modes, freqs, samples, 2, base), BF16),
            pltpu.SemaphoreType.DMA(e_kept.shape[:2]),
            pltpu.SemaphoreType.DMA((modes,)),
            pltpu.SemaphoreType.DMA((modes, freqs)),
        ],
        name="back",
        cost_estimate=cost(8 * modes * samples * freqs * base * kmax, e, e),
        compiler_params=limit(MIB * 16),
    )(place, retained, stats, *quarters, e_kept, pltpu.with_memory_space_constraint(e, pltpu.HBM))


def per_device(visibilities, eigenmodes, retained):
    freq_size, ma_size = lax.axis_size("freq"), lax.axis_size("ma")
    index = lax.axis_index("freq").astype(jnp.int32)
    place = jnp.stack([index & 1, (index >> 1) & 1])

    def swap(x, bits):
        return lax.ppermute(x, "freq", [(i, i ^ bits) for i in range(freq_size)])

    given, kept, e_kept = project(place, visibilities, eigenmodes)
    total = kept + swap(given, 1).astype(F32)
    leaves, mine = total[0].astype(BF16), total[1]
    theirs = swap(leaves, 2)
    bit = 4
    while bit < freq_size:
        mine = mine + theirs.astype(F32)
        theirs = swap(mine.astype(BF16), bit)
        bit *= 2
    quarter, stats = power_of(place, retained, mine, theirs, ma_size * freq_size)
    stats = lax.all_to_all(stats, ("ma", "freq"), 0, 0, tiled=True)
    quarters = [quarter] + [swap(quarter, bits) for bits in (1, 2, 3)]
    return tuple(back(place, retained, freq_size, stats, quarters, e_kept, eigenmodes))


def solution(mesh):
    return jax.shard_map(
        per_device,
        mesh=mesh,
        in_specs=(P("ma", None, "freq", None, None), P("ma", "freq", None, None, None), P("ma")),
        out_specs=(P("ma", None, None, None), P("ma", None, "freq", None, None)),
        check_vma=False,
    )
```

```python
import functools

import jax
import jax.numpy as jnp
from jax import lax
from jax.experimental import pallas as pl
from jax.experimental.pallas import tpu as pltpu
from jax.sharding import PartitionSpec as P

F32 = jnp.float32
BF16 = jnp.bfloat16
TOTAL = F32
VMEM = pl.BlockSpec(memory_space=pltpu.VMEM)
HBM = pl.BlockSpec(memory_space=pltpu.HBM)
MIB = 1 << 20


def limit(vmem):
    return pltpu.CompilerParams(vmem_limit_bytes=vmem)


def side():
    return (lax.axis_index("freq") & 1).astype(jnp.int32)


def times_i(x):
    up = pltpu.roll(x, x.shape[0] - 1, 0)
    down = pltpu.roll(x, 1, 0)
    even = (lax.broadcasted_iota(jnp.int32, x.shape, 0) & 1) == 0
    return jnp.where(even, -up, down)


def project_kernel(v_hbm, e_hbm, given_ref, kept_ref, e_ref, v_buf, acc, v_sem, e_sem):
    modes, freqs, samples, _, base = v_buf.shape
    rows = 2 * samples
    half = modes // 2
    mode = [lax.rem((1 - side()) * half + j, modes) for j in range(modes)]
    copies = []
    for j in range(modes):
        for f in range(freqs):
            e_copy = pltpu.make_async_copy(e_hbm.at[mode[j], f], e_ref.at[mode[j], f], e_sem.at[j, f])
            v_copy = pltpu.make_async_copy(v_hbm.at[mode[j], :, f], v_buf.at[j, f], v_sem.at[j, f])
            e_copy.start()
            v_copy.start()
            copies.append((e_copy, v_copy))
    for j in range(modes):
        for f in range(freqs):
            for copy in copies[j * freqs + f]:
                copy.wait()
            x = v_buf[j, f].reshape(rows, base)
            by_re = jnp.dot(x, e_ref[mode[j], f, 0], preferred_element_type=F32)
            by_im = jnp.dot(x, e_ref[mode[j], f, 1], preferred_element_type=F32)
            if f > 0:
                by_re += acc[0]
                by_im += acc[1]
            if f < freqs - 1:
                acc[0] = by_re
                acc[1] = by_im
            else:
                out_ref = given_ref if j < half else kept_ref
                out = by_re - times_i(by_im)
                out_ref[pl.ds(j % half * rows, rows), :] = out.astype(out_ref.dtype)


def project(v, e):
    modes, samples, freqs, _, base = v.shape
    kmax = e.shape[-1]
    rows = modes // 2 * 2 * samples
    return pl.pallas_call(
        project_kernel,
        in_specs=[HBM, HBM],
        out_specs=[VMEM, VMEM, VMEM],
        out_shape=[
            jax.ShapeDtypeStruct((rows, kmax), BF16),
            jax.ShapeDtypeStruct((rows, kmax), F32),
            jax.ShapeDtypeStruct(e.shape, e.dtype),
        ],
        scratch_shapes=[
            pltpu.VMEM((modes, freqs, samples, 2, base), v.dtype),
            pltpu.VMEM((2, 2 * samples, kmax), F32),
            pltpu.SemaphoreType.DMA((modes, freqs)),
            pltpu.SemaphoreType.DMA((modes, freqs)),
        ],
        name="project",
        compiler_params=limit(MIB * 16),
    )(pltpu.with_memory_space_constraint(v, pltpu.HBM), pltpu.with_memory_space_constraint(e, pltpu.HBM))


def power_kernel(keep_ref, mine_ref, theirs_ref, total_ref, stats_ref):
    half = keep_ref.shape[0] // 2
    kmax = mine_ref.shape[1]
    rows = mine_ref.shape[0] // half
    stats = jnp.zeros((2, kmax), F32)
    for j in range(half):
        at = pl.ds(j * rows, rows)
        total = mine_ref[at, :].astype(F32) + theirs_ref[at, :].astype(F32)
        total_ref[at, :] = total.astype(total_ref.dtype)
        keep = jnp.where(side() == 0, keep_ref[j : j + 1], keep_ref[half + j : half + j + 1])
        power = keep * jnp.sum(total * total, axis=0, keepdims=True)
        stats += jnp.concatenate([power, keep], axis=0)
    stats_ref[...] = jnp.broadcast_to(stats[None], stats_ref.shape)


def power_of(keep, mine, theirs, peers):
    rows, kmax = mine.shape
    return pl.pallas_call(
        power_kernel,
        in_specs=[VMEM, VMEM, VMEM],
        out_specs=[VMEM, VMEM],
        out_shape=[
            jax.ShapeDtypeStruct((rows, kmax), TOTAL),
            jax.ShapeDtypeStruct((peers, 2, kmax), F32),
        ],
        name="power",
        compiler_params=limit(MIB * 4),
    )(keep, mine, theirs)


def back_kernel(
    copies, keep_ref, stats_ref, mine_ref, other_ref, e_ref, coef_hbm, out_hbm, pair, flat, coef_buf, out_buf, coef_sem, out_sem
):
    modes, freqs, samples, _, base = out_buf.shape
    kmax = mine_ref.shape[1]
    rows = 2 * samples
    half = modes // 2
    lanes = flat.shape[2]
    stats = jnp.sum(stats_ref[...], axis=0) * F32(1.0 / copies)
    power, count = stats[0:1], F32(samples) * stats[1:2]
    scale = 1.0 / jnp.sqrt(power / jnp.maximum(count, 1.0) + 1e-06)
    contract = (((1,), (1,)), ((), ()))
    pending = []
    for j in range(modes):
        mode = lax.rem(side() * half + j, modes)
        proj_ref = mine_ref if j < half else other_ref
        other = (j + half) % modes
        gain = jnp.where(side() == 0, keep_ref[j : j + 1], keep_ref[other : other + 1]) * scale
        coef = proj_ref[pl.ds(j % half * rows, rows), :].astype(F32) * gain
        pair[:, :kmax] = coef.astype(BF16)
        pair[:, kmax:] = times_i(coef).astype(BF16)
        for i in range(kmax // lanes):
            flat[i] = coef[:, i * lanes : (i + 1) * lanes]
            for part in range(2):
                every = flat[i, pl.ds(part, samples, stride=2), :]
                coef_buf[j, part, :, i * lanes : (i + 1) * lanes] = every.astype(BF16)
        copy = pltpu.make_async_copy(coef_buf.at[j], coef_hbm.at[mode], coef_sem.at[j])
        copy.start()
        pending.append(copy)
        for f in range(freqs):
            out = lax.dot_general(pair[:, :kmax], e_ref[mode, f, 0], contract, preferred_element_type=F32)
            out += lax.dot_general(pair[:, kmax:], e_ref[mode, f, 1], contract, preferred_element_type=F32)
            out_buf[j, f] = out.astype(BF16).reshape(samples, 2, base)
            copy = pltpu.make_async_copy(out_buf.at[j, f], out_hbm.at[mode, :, f], out_sem.at[j, f])
            copy.start()
            pending.append(copy)
    for copy in pending:
        copy.wait()


def back(keep, copies, stats, mine, other, e):
    kmax = mine.shape[1]
    modes, freqs, _, base, _ = e.shape
    samples = mine.shape[0] // modes
    return pl.pallas_call(
        functools.partial(back_kernel, copies),
        in_specs=[VMEM] * 5,
        out_specs=[HBM, HBM],
        out_shape=[
            jax.ShapeDtypeStruct((modes, 2, samples, kmax), BF16),
            jax.ShapeDtypeStruct((modes, samples, freqs, 2, base), BF16),
        ],
        scratch_shapes=[
            pltpu.VMEM((2 * samples, 2 * kmax), BF16),
            pltpu.VMEM((kmax // 128, 2 * samples, 128), F32),
            pltpu.VMEM((modes, 2, samples, kmax), BF16),
            pltpu.VMEM((modes, freqs, samples, 2, base), BF16),
            pltpu.SemaphoreType.DMA((modes,)),
            pltpu.SemaphoreType.DMA((modes, freqs)),
        ],
        name="back",
        compiler_params=limit(MIB * 16),
    )(keep, stats, mine, other, e)


def per_device(visibilities, eigenmodes, retained):
    freq_size, ma_size = lax.axis_size("freq"), lax.axis_size("ma")
    ranks = jnp.arange(eigenmodes.shape[-1], dtype=jnp.int32)
    keep = (ranks[None, :] < retained[:, None]).astype(F32)

    def swap(x, bit):
        return lax.ppermute(x, "freq", [(i, i ^ bit) for i in range(freq_size)])

    given, kept, e_vmem = project(visibilities, eigenmodes)
    total = (kept + swap(given, 1).astype(F32)).astype(BF16)
    bit = 2
    while 2 * bit < freq_size:
        total = (total.astype(F32) + swap(total, bit).astype(F32)).astype(BF16)
        bit *= 2
    mine, stats = power_of(keep, total, swap(total, bit), ma_size * freq_size)
    other = swap(mine, 1)
    stats = lax.all_to_all(stats, ("ma", "freq"), 0, 0, tiled=True)
    coefficients, filtered = back(keep, freq_size // 2, stats, mine, other, e_vmem)
    return coefficients, filtered


def solution(mesh):
    return jax.shard_map(
        per_device,
        mesh=mesh,
        in_specs=(P("ma", None, "freq", None, None), P("ma", "freq", None, None, None), P("ma")),
        out_specs=(P("ma", None, None, None), P("ma", None, "freq", None, None)),
        check_vma=False,
    )
```

```python
import functools

import jax
import jax.numpy as jnp
from jax import lax
from jax.experimental import pallas as pl
from jax.experimental.pallas import tpu as pltpu
from jax.sharding import PartitionSpec as P

F32 = jnp.float32
BF16 = jnp.bfloat16
VMEM = pl.BlockSpec(memory_space=pltpu.VMEM)
HBM = pl.BlockSpec(memory_space=pltpu.HBM)
MIB = 1 << 20


def limit(vmem):
    return pltpu.CompilerParams(vmem_limit_bytes=vmem)


def cost(flops, *arrays):
    moved = sum(a.size * a.dtype.itemsize for a in arrays)
    return pl.CostEstimate(flops=flops, bytes_accessed=moved, transcendentals=0)


def side():
    return (lax.axis_index("freq") & 1).astype(jnp.int32)


def times_i(x):
    up = pltpu.roll(x, x.shape[0] - 1, 0)
    down = pltpu.roll(x, 1, 0)
    even = (lax.broadcasted_iota(jnp.int32, x.shape, 0) & 1) == 0
    return jnp.where(even, -up, down)


def finish(j, by_re, by_im, give_ref, keep_ref):
    out = by_re - times_i(by_im)
    half = out.shape[0] // 2
    low, high = out[:half], out[half:]
    give_ref[j] = jnp.where(side() == 0, high, low).astype(give_ref.dtype)
    keep_ref[j] = jnp.where(side() == 0, low, high).astype(keep_ref.dtype)


def project_kernel(v_hbm, e_hbm, give_ref, keep_ref, part_ref, v_last, e_ref, v_buf, acc, v_sem, e_sem):
    modes, freqs = v_sem.shape
    samples, _, base = v_buf.shape[2:]
    half = modes // 2
    copies = []
    for m in range(modes):
        for f in range(freqs):
            late = m >= half and f == freqs - 1
            v_to = v_last.at[m - half] if late else v_buf.at[m, f]
            e_copy = pltpu.make_async_copy(e_hbm.at[m, f], e_ref.at[m, f], e_sem.at[m, f])
            v_copy = pltpu.make_async_copy(v_hbm.at[m, :, f], v_to, v_sem.at[m, f])
            e_copy.start()
            v_copy.start()
            copies.append((e_copy, v_copy))
    for m in range(modes):
        for f in range(freqs):
            for copy in copies[m * freqs + f]:
                copy.wait()
            if m >= half and f == freqs - 1:
                continue
            x = v_buf[m, f].reshape(2 * samples, base)
            by_re = jnp.dot(x, e_ref[m, f, 0], preferred_element_type=F32)
            by_im = jnp.dot(x, e_ref[m, f, 1], preferred_element_type=F32)
            sums = part_ref.at[m - half] if m >= half else acc
            if f > 0:
                by_re += sums[0]
                by_im += sums[1]
            if m >= half or f < freqs - 1:
                sums[0] = by_re
                sums[1] = by_im
            else:
                finish(m, by_re, by_im, give_ref, keep_ref)


def project(v, e):
    modes, samples, freqs, _, base = v.shape
    kmax = e.shape[-1]
    half = modes // 2
    return pl.pallas_call(
        project_kernel,
        in_specs=[HBM, HBM],
        out_specs=[VMEM] * 5,
        out_shape=[
            jax.ShapeDtypeStruct((half, samples, kmax), BF16),
            jax.ShapeDtypeStruct((half, samples, kmax), F32),
            jax.ShapeDtypeStruct((half, 2, 2 * samples, kmax), F32),
            jax.ShapeDtypeStruct((half, samples, 2, base), v.dtype),
            jax.ShapeDtypeStruct(e.shape, e.dtype),
        ],
        scratch_shapes=[
            pltpu.VMEM((modes, freqs, samples, 2, base), v.dtype),
            pltpu.VMEM((2, 2 * samples, kmax), F32),
            pltpu.SemaphoreType.DMA((modes, freqs)),
            pltpu.SemaphoreType.DMA((modes, freqs)),
        ],
        name="project",
        compiler_params=limit(MIB * 16),
        cost_estimate=cost(8 * modes * samples * freqs * base * kmax, v, e),
    )(pltpu.with_memory_space_constraint(v, pltpu.HBM), pltpu.with_memory_space_constraint(e, pltpu.HBM))


def rest_kernel(part_ref, v_ref, e_ref, give_ref, keep_ref):
    modes, freqs = e_ref.shape[:2]
    half, samples, _, base = v_ref.shape
    for j in range(half):
        x = v_ref[j].reshape(2 * samples, base)
        by_re = part_ref[j, 0] + jnp.dot(x, e_ref[half + j, freqs - 1, 0], preferred_element_type=F32)
        by_im = part_ref[j, 1] + jnp.dot(x, e_ref[half + j, freqs - 1, 1], preferred_element_type=F32)
        finish(j, by_re, by_im, give_ref, keep_ref)


def rest(part, v, e):
    half, samples, _, base = v.shape
    kmax = e.shape[-1]
    return pl.pallas_call(
        rest_kernel,
        in_specs=[VMEM] * 3,
        out_specs=[VMEM] * 2,
        out_shape=[
            jax.ShapeDtypeStruct((half, samples, kmax), BF16),
            jax.ShapeDtypeStruct((half, samples, kmax), F32),
        ],
        name="rest",
        compiler_params=limit(MIB * 4),
        cost_estimate=cost(8 * half * samples * base * kmax, v),
    )(part, v, e)


def power_kernel(keep_ref, a_ref, a_their_ref, b_ref, b_their_ref, total_ref, stats_ref):
    half, _, kmax = a_ref.shape
    stats = jnp.zeros((2, kmax), F32)
    for m in range(2 * half):
        mine, theirs = (a_ref, a_their_ref) if m < half else (b_ref, b_their_ref)
        total = mine[m % half].astype(F32) + theirs[m % half].astype(F32)
        total_ref[m] = total
        keep = keep_ref[m : m + 1]
        power = keep * jnp.sum(total * total, axis=0, keepdims=True)
        stats += jnp.concatenate([power, keep], axis=0)
    stats_ref[...] = jnp.broadcast_to(stats[None], stats_ref.shape)


def power_of(keep, pairs, peers):
    half, rows, kmax = pairs[0].shape
    return pl.pallas_call(
        power_kernel,
        in_specs=[VMEM] * 5,
        out_specs=[VMEM] * 2,
        out_shape=[
            jax.ShapeDtypeStruct((2 * half, rows, kmax), F32),
            jax.ShapeDtypeStruct((peers, 2, kmax), F32),
        ],
        name="power",
        compiler_params=limit(MIB * 4),
    )(keep, *pairs)


def back_kernel(
    freq_size, keep_ref, stats_ref, mine_ref, other_ref, e_ref, coef_hbm, out_hbm, pair, flat, coef_buf, out_buf, coef_sem, out_sem
):
    modes, freqs, samples, _, base = out_buf.shape
    kmax = mine_ref.shape[-1]
    lanes = flat.shape[2]
    stats = jnp.sum(stats_ref[...], axis=0)
    power, count = stats[0:1] * F32(2 / freq_size), F32(samples) * (stats[1:2] * F32(1 / freq_size))
    scale = 1.0 / jnp.sqrt(power / jnp.maximum(count, 1.0) + 1e-06)
    contract = (((1,), (1,)), ((), ()))
    pending = []

    def send(src, dst, sem):
        copy = pltpu.make_async_copy(src, dst, sem)
        copy.start()
        pending.append(copy)

    for m in range(modes):
        gain = keep_ref[m : m + 1] * scale
        mine, other = mine_ref[m] * gain, other_ref[m] * gain
        for h in range(2):
            coef = jnp.where(side() == h, mine, other)
            at = slice(h * samples, (h + 1) * samples)
            pair[at, :kmax] = coef.astype(BF16)
            pair[at, kmax:] = times_i(coef).astype(BF16)
            for i in range(kmax // lanes):
                flat[i, at, :] = coef[:, i * lanes : (i + 1) * lanes]
        for f in range(freqs):
            out = lax.dot_general(pair[:, :kmax], e_ref[m, f, 0], contract, preferred_element_type=F32)
            out += lax.dot_general(pair[:, kmax:], e_ref[m, f, 1], contract, preferred_element_type=F32)
            out_buf[m, f] = out.astype(BF16).reshape(samples, 2, base)
            if f == 0:
                for i in range(kmax // lanes):
                    for part in range(2):
                        every = flat[i, pl.ds(part, samples, stride=2), :]
                        coef_buf[m, part, :, i * lanes : (i + 1) * lanes] = every.astype(BF16)
                send(coef_buf.at[m], coef_hbm.at[m], coef_sem.at[m])
            send(out_buf.at[m, f], out_hbm.at[m, :, f], out_sem.at[m, f])
    for copy in pending:
        copy.wait()


def back(keep, freq_size, stats, mine, other, e):
    modes, freqs, _, base, kmax = e.shape
    samples = mine.shape[1]
    return pl.pallas_call(
        functools.partial(back_kernel, freq_size),
        in_specs=[VMEM] * 5,
        out_specs=[HBM, HBM],
        out_shape=[
            jax.ShapeDtypeStruct((modes, 2, samples, kmax), BF16),
            jax.ShapeDtypeStruct((modes, samples, freqs, 2, base), BF16),
        ],
        scratch_shapes=[
            pltpu.VMEM((2 * samples, 2 * kmax), BF16),
            pltpu.VMEM((kmax // 128, 2 * samples, 128), F32),
            pltpu.VMEM((modes, 2, samples, kmax), BF16),
            pltpu.VMEM((modes, freqs, samples, 2, base), BF16),
            pltpu.SemaphoreType.DMA((modes,)),
            pltpu.SemaphoreType.DMA((modes, freqs)),
        ],
        name="back",
        compiler_params=limit(MIB * 16),
    )(keep, stats, mine, other, e)


def per_device(visibilities, eigenmodes, retained):
    freq_size, ma_size = lax.axis_size("freq"), lax.axis_size("ma")
    ranks = jnp.arange(eigenmodes.shape[-1], dtype=jnp.int32)
    keep = (ranks[None, :] < retained[:, None]).astype(F32)

    def swap(x, bit):
        return lax.ppermute(x, "freq", [(i, i ^ bit) for i in range(freq_size)])

    give_a, keep_a, part, v_last, e_vmem = project(visibilities, eigenmodes)
    give_b, keep_b = rest(part, v_last, e_vmem)
    pairs = []
    for give, kept in ((give_a, keep_a), (give_b, keep_b)):
        total = (kept + swap(give, 1).astype(F32)).astype(BF16)
        bit = 2
        while 2 * bit < freq_size:
            total = (total.astype(F32) + swap(total, bit).astype(F32)).astype(BF16)
            bit *= 2
        pairs += [total, swap(total, bit)]
    mine, stats = power_of(keep, pairs, ma_size * freq_size)
    other = swap(mine, 1)
    stats = lax.all_to_all(stats, ("ma", "freq"), 0, 0, tiled=True)
    return tuple(back(keep, freq_size, stats, mine, other, e_vmem))


def solution(mesh):
    return jax.shard_map(
        per_device,
        mesh=mesh,
        in_specs=(P("ma", None, "freq", None, None), P("ma", "freq", None, None, None), P("ma")),
        out_specs=(P("ma", None, None, None), P("ma", None, "freq", None, None)),
        check_vma=False,
    )
```

```python
import functools

import jax
import jax.numpy as jnp
from jax import lax
from jax.experimental import pallas as pl
from jax.experimental.pallas import tpu as pltpu
from jax.sharding import PartitionSpec as P


F32 = jnp.float32
BF16 = jnp.bfloat16
VMEM = pl.BlockSpec(memory_space=pltpu.VMEM)
HBM = pl.BlockSpec(memory_space=pltpu.HBM)
MIB = 1 << 20


def limit(vmem):
    return pltpu.CompilerParams(vmem_limit_bytes=vmem)


def cost(flops, *arrays):
    moved = sum(a.size * a.dtype.itemsize for a in arrays)
    return pl.CostEstimate(flops=flops, bytes_accessed=moved, transcendentals=0)


def side(bit=0):
    return ((lax.axis_index("freq") >> bit) & 1).astype(jnp.int32)


def times_i(x):
    up = pltpu.roll(x, x.shape[0] - 1, 0)
    down = pltpu.roll(x, 1, 0)
    even = (lax.broadcasted_iota(jnp.int32, x.shape, 0) & 1) == 0
    return jnp.where(even, -up, down)


def finish(j, by_re, by_im, give_ref, keep_ref):
    out = by_re - times_i(by_im)
    half = out.shape[0] // 2
    low, high = out[:half], out[half:]
    give_ref[j] = jnp.where(side() == 0, high, low).astype(give_ref.dtype)
    keep_ref[j] = jnp.where(side() == 0, low, high).astype(keep_ref.dtype)


def project_kernel(v_hbm, e_hbm, give_ref, keep_ref, part_ref, v_last, e_ref, v_buf, acc, v_sem, e_sem):
    modes, freqs = v_sem.shape
    samples, _, base = v_buf.shape[2:]
    half = modes // 2
    copies = []
    for m in range(modes):
        for f in range(freqs):
            late = m >= half and f == freqs - 1
            v_to = v_last.at[m - half] if late else v_buf.at[m, f]
            e_copy = pltpu.make_async_copy(e_hbm.at[m, f], e_ref.at[m, f], e_sem.at[m, f])
            v_copy = pltpu.make_async_copy(v_hbm.at[m, :, f], v_to, v_sem.at[m, f])
            e_copy.start()
            v_copy.start()
            copies.append((e_copy, v_copy))
    for m in range(modes):
        for f in range(freqs):
            for copy in copies[m * freqs + f]:
                copy.wait()
            if m >= half and f == freqs - 1:
                continue
            x = v_buf[m, f].reshape(2 * samples, base)
            by_re = jnp.dot(x, e_ref[m, f, 0], preferred_element_type=F32)
            by_im = jnp.dot(x, e_ref[m, f, 1], preferred_element_type=F32)
            sums = part_ref.at[m - half] if m >= half else acc
            if f > 0:
                by_re += sums[0]
                by_im += sums[1]
            if m >= half or f < freqs - 1:
                sums[0] = by_re
                sums[1] = by_im
            else:
                finish(m, by_re, by_im, give_ref, keep_ref)


def project(v, e):
    modes, samples, freqs, _, base = v.shape
    kmax = e.shape[-1]
    half = modes // 2
    return pl.pallas_call(
        project_kernel,
        in_specs=[HBM, HBM],
        out_specs=[VMEM] * 5,
        out_shape=[
            jax.ShapeDtypeStruct((half, samples, kmax), BF16),
            jax.ShapeDtypeStruct((half, samples, kmax), F32),
            jax.ShapeDtypeStruct((half, 2, 2 * samples, kmax), F32),
            jax.ShapeDtypeStruct((half, samples, 2, base), v.dtype),
            jax.ShapeDtypeStruct(e.shape, e.dtype),
        ],
        scratch_shapes=[
            pltpu.VMEM((modes, freqs, samples, 2, base), v.dtype),
            pltpu.VMEM((2, 2 * samples, kmax), F32),
            pltpu.SemaphoreType.DMA((modes, freqs)),
            pltpu.SemaphoreType.DMA((modes, freqs)),
        ],
        name="project",
        compiler_params=limit(MIB * 16),
        cost_estimate=cost(8 * modes * samples * freqs * base * kmax, v, e),
    )(pltpu.with_memory_space_constraint(v, pltpu.HBM), pltpu.with_memory_space_constraint(e, pltpu.HBM))


def rest_kernel(part_ref, v_ref, e_ref, give_ref, keep_ref):
    _, freqs = e_ref.shape[:2]
    half, samples, _, base = v_ref.shape
    for j in range(half):
        x = v_ref[j].reshape(2 * samples, base)
        by_re = part_ref[j, 0] + jnp.dot(x, e_ref[half + j, freqs - 1, 0], preferred_element_type=F32)
        by_im = part_ref[j, 1] + jnp.dot(x, e_ref[half + j, freqs - 1, 1], preferred_element_type=F32)
        finish(j, by_re, by_im, give_ref, keep_ref)


def rest(part, v, e):
    half, samples, _, base = v.shape
    kmax = e.shape[-1]
    return pl.pallas_call(
        rest_kernel,
        in_specs=[VMEM] * 3,
        out_specs=[VMEM] * 2,
        out_shape=[
            jax.ShapeDtypeStruct((half, samples, kmax), BF16),
            jax.ShapeDtypeStruct((half, samples, kmax), F32),
        ],
        name="rest",
        compiler_params=limit(MIB * 4),
        cost_estimate=cost(8 * half * samples * base * kmax, v),
    )(part, v, e)


def split_kernel(mine_ref, theirs_ref, give_ref, keep_ref):
    half, rows, _ = give_ref.shape
    for j in range(half):
        total = mine_ref[j] + theirs_ref[j].astype(F32)
        low, high = total[:rows], total[rows:]
        give_ref[j] = jnp.where(side(1) == 0, high, low).astype(give_ref.dtype)
        keep_ref[j] = jnp.where(side(1) == 0, low, high)


def split(mine, theirs):
    half, rows, kmax = mine.shape
    return pl.pallas_call(
        split_kernel,
        in_specs=[VMEM] * 2,
        out_specs=[VMEM] * 2,
        out_shape=[
            jax.ShapeDtypeStruct((half, rows // 2, kmax), BF16),
            jax.ShapeDtypeStruct((half, rows // 2, kmax), F32),
        ],
        name="split",
        compiler_params=limit(MIB * 2),
    )(mine, theirs)


def power_kernel(freq_size, keep_ref, quarter_ref, b_ref, b_their_ref, total_ref, stats_ref):
    half, _, kmax = b_ref.shape
    stats = jnp.zeros((2, kmax), F32)
    for m in range(2 * half):
        if m < half:
            total, copies = quarter_ref[m].astype(F32), freq_size // 4
        else:
            total, copies = b_ref[m - half].astype(F32) + b_their_ref[m - half].astype(F32), freq_size // 2
            total_ref[m - half] = total
        keep = keep_ref[m : m + 1]
        power = keep * jnp.sum(total * total, axis=0, keepdims=True) * F32(1.0 / copies)
        stats += jnp.concatenate([power, keep * F32(1.0 / freq_size)], axis=0)
    stats_ref[...] = jnp.broadcast_to(stats[None], stats_ref.shape)


def power_of(keep, freq_size, quarter, mine, theirs, peers):
    kmax = mine.shape[-1]
    return pl.pallas_call(
        functools.partial(power_kernel, freq_size),
        in_specs=[VMEM] * 4,
        out_specs=[VMEM] * 2,
        out_shape=[
            jax.ShapeDtypeStruct(mine.shape, F32),
            jax.ShapeDtypeStruct((peers, 2, kmax), F32),
        ],
        name="power",
        compiler_params=limit(MIB * 4),
    )(keep, quarter, mine, theirs)


def pool_kernel(samples, stats_ref, scale_ref):
    stats = jnp.sum(stats_ref[...], axis=0)
    power, count = stats[0:1], F32(samples) * stats[1:2]
    scale_ref[...] = 1.0 / jnp.sqrt(power / jnp.maximum(count, 1.0) + 1e-06)


def pool(stats, samples):
    return pl.pallas_call(
        functools.partial(pool_kernel, samples),
        in_specs=[VMEM],
        out_specs=VMEM,
        out_shape=jax.ShapeDtypeStruct((1, stats.shape[-1]), F32),
        name="pool",
        compiler_params=limit(MIB),
    )(stats)


def pieces(m, c, y, quarters, mine_ref, other_ref):
    half = mine_ref.shape[0]
    if m < half:
        own, core, chip, both = [q[m].astype(F32) for q in quarters]
        rows = own.shape[0]
        for c_of in range(2):
            near, far = jnp.where(c == c_of, own, core), jnp.where(c == c_of, chip, both)
            for y_of in range(2):
                yield (2 * c_of + y_of) * rows, jnp.where(y == y_of, near, far)
    else:
        mine, other = mine_ref[m - half], other_ref[m - half]
        for c_of in range(2):
            yield c_of * mine.shape[0], jnp.where(c == c_of, mine, other)


def back_kernel(
    keep_ref, scale_ref, q0_ref, q1_ref, q2_ref, q3_ref, mine_ref, other_ref, e_ref, coef_hbm, out_hbm, pair, flat, coef_buf, out_buf, coef_sem, out_sem
):
    modes, freqs, samples, _, base = out_buf.shape
    kmax = mine_ref.shape[-1]
    lanes = flat.shape[2]
    contract = (((1,), (1,)), ((), ()))
    pending = []

    def send(src, dst, sem):
        copy = pltpu.make_async_copy(src, dst, sem)
        copy.start()
        pending.append(copy)

    for m in range(modes):
        gain = keep_ref[m : m + 1] * scale_ref[...]
        for start, proj in pieces(m, side(), side(1), (q0_ref, q1_ref, q2_ref, q3_ref), mine_ref, other_ref):
            coef = proj * gain
            at = slice(start, start + coef.shape[0])
            pair[at, :kmax] = coef.astype(BF16)
            pair[at, kmax:] = times_i(coef).astype(BF16)
            for i in range(kmax // lanes):
                flat[i, at, :] = coef[:, i * lanes : (i + 1) * lanes]
        for f in range(freqs):
            out = lax.dot_general(pair[:, :kmax], e_ref[m, f, 0], contract, preferred_element_type=F32)
            out += lax.dot_general(pair[:, kmax:], e_ref[m, f, 1], contract, preferred_element_type=F32)
            out_buf[m, f] = out.astype(BF16).reshape(samples, 2, base)
            if f == 0:
                for i in range(kmax // lanes):
                    for part in range(2):
                        every = flat[i, pl.ds(part, samples, stride=2), :]
                        coef_buf[m, part, :, i * lanes : (i + 1) * lanes] = every.astype(BF16)
                send(coef_buf.at[m], coef_hbm.at[m], coef_sem.at[m])
            send(out_buf.at[m, f], out_hbm.at[m, :, f], out_sem.at[m, f])
    for copy in pending:
        copy.wait()


def back(keep, scale, quarters, mine, other, e):
    modes, freqs, _, base, kmax = e.shape
    samples = mine.shape[1]
    return pl.pallas_call(
        back_kernel,
        in_specs=[VMEM] * 9,
        out_specs=[HBM, HBM],
        out_shape=[
            jax.ShapeDtypeStruct((modes, 2, samples, kmax), BF16),
            jax.ShapeDtypeStruct((modes, samples, freqs, 2, base), BF16),
        ],
        scratch_shapes=[
            pltpu.VMEM((2 * samples, 2 * kmax), BF16),
            pltpu.VMEM((kmax // 128, 2 * samples, 128), F32),
            pltpu.VMEM((modes, 2, samples, kmax), BF16),
            pltpu.VMEM((modes, freqs, samples, 2, base), BF16),
            pltpu.SemaphoreType.DMA((modes,)),
            pltpu.SemaphoreType.DMA((modes, freqs)),
        ],
        name="back",
        compiler_params=limit(MIB * 16),
    )(keep, scale, *quarters, mine, other, e)


def filter_modes(visibilities, eigenmodes, retained):
    freq_size, ma_size = lax.axis_size("freq"), lax.axis_size("ma")
    ranks = jnp.arange(eigenmodes.shape[-1], dtype=jnp.int32)
    keep = (ranks[None, :] < retained[:, None]).astype(F32)

    def swap(x, bit):
        return lax.ppermute(x, "freq", [(i, i ^ bit) for i in range(freq_size)])

    def over_chips(total):
        bit = 2
        while 2 * bit < freq_size:
            total = (total.astype(F32) + swap(total, bit).astype(F32)).astype(BF16)
            bit *= 2
        return total, swap(total, bit)

    give_a, keep_a, part, v_last, e_vmem = project(visibilities, eigenmodes)
    give_b, keep_b = rest(part, v_last, e_vmem)
    give_a, keep_a = split(keep_a, swap(give_a, 1))
    quarter = keep_a + swap(give_a, 2).astype(F32)
    bit = 4
    while bit < freq_size:
        quarter = quarter + swap(quarter.astype(BF16), bit).astype(F32)
        bit *= 2
    quarter = quarter.astype(BF16)
    total, theirs = over_chips((keep_b + swap(give_b, 1).astype(F32)).astype(BF16))
    quarters = [quarter]
    for bits in (1, 2, 3):
        quarters.append(swap(quarter, bits))
    mine, stats = power_of(keep, freq_size, quarter, total, theirs, ma_size * freq_size)
    other = swap(mine, 1)
    scale = pool(lax.all_to_all(stats, ("ma", "freq"), 0, 0, tiled=True), visibilities.shape[1])
    return tuple(back(keep, scale, quarters, mine, other, e_vmem))


def solution(mesh):
    return jax.shard_map(
        filter_modes,
        mesh=mesh,
        in_specs=(P("ma", None, "freq", None, None), P("ma", "freq", None, None, None), P("ma")),
        out_specs=(P("ma", None, None, None), P("ma", None, "freq", None, None)),
        check_vma=False,
    )
```

```python
import functools

import jax
import jax.numpy as jnp
from jax import lax
from jax.experimental import pallas as pl
from jax.experimental.pallas import tpu as pltpu
from jax.sharding import PartitionSpec as P

F32 = jnp.float32
BF16 = jnp.bfloat16
VMEM = pl.BlockSpec(memory_space=pltpu.VMEM)
HBM = pl.BlockSpec(memory_space=pltpu.HBM)
MIB = 1 << 20


def limit(vmem):
    return pltpu.CompilerParams(vmem_limit_bytes=vmem)


def cost(flops, *arrays):
    moved = sum(a.size * a.dtype.itemsize for a in arrays)
    return pl.CostEstimate(flops=flops, bytes_accessed=moved, transcendentals=0)


def side():
    return (lax.axis_index("freq") & 1).astype(jnp.int32)


def times_i(x):
    up = pltpu.roll(x, x.shape[0] - 1, 0)
    down = pltpu.roll(x, 1, 0)
    even = (lax.broadcasted_iota(jnp.int32, x.shape, 0) & 1) == 0
    return jnp.where(even, -up, down)


def finish(j, by_re, by_im, give_ref, keep_ref):
    out = by_re - times_i(by_im)
    give_ref[j] = out.astype(give_ref.dtype)
    keep_ref[j] = out.astype(keep_ref.dtype)


def project_kernel(v_hbm, e_hbm, give_ref, keep_ref, part_ref, v_last, e_ref, v_buf, acc, v_sem, e_sem):
    modes, freqs = v_sem.shape
    samples, _, base = v_buf.shape[2:]
    half = modes // 2
    copies = []
    for m in range(modes):
        for f in range(freqs):
            late = m >= half and f == freqs - 1
            v_to = v_last.at[m - half] if late else v_buf.at[m, f]
            e_copy = pltpu.make_async_copy(e_hbm.at[m, f], e_ref.at[m, f], e_sem.at[m, f])
            v_copy = pltpu.make_async_copy(v_hbm.at[m, :, f], v_to, v_sem.at[m, f])
            e_copy.start()
            v_copy.start()
            copies.append((e_copy, v_copy))
    for m in range(modes):
        for f in range(freqs):
            for copy in copies[m * freqs + f]:
                copy.wait()
            if m >= half and f == freqs - 1:
                continue
            x = v_buf[m, f].reshape(2 * samples, base)
            by_re = jnp.dot(x, e_ref[m, f, 0], preferred_element_type=F32)
            by_im = jnp.dot(x, e_ref[m, f, 1], preferred_element_type=F32)
            sums = part_ref.at[m - half] if m >= half else acc
            if f > 0:
                by_re += sums[0]
                by_im += sums[1]
            if m >= half or f < freqs - 1:
                sums[0] = by_re
                sums[1] = by_im
            else:
                finish(m, by_re, by_im, give_ref, keep_ref)


def project(v, e):
    modes, samples, freqs, _, base = v.shape
    kmax = e.shape[-1]
    half = modes // 2
    return pl.pallas_call(
        project_kernel,
        in_specs=[HBM, HBM],
        out_specs=[VMEM] * 5,
        out_shape=[
            jax.ShapeDtypeStruct((half, 2 * samples, kmax), BF16),
            jax.ShapeDtypeStruct((half, 2 * samples, kmax), F32),
            jax.ShapeDtypeStruct((half, 2, 2 * samples, kmax), F32),
            jax.ShapeDtypeStruct((half, samples, 2, base), v.dtype),
            jax.ShapeDtypeStruct(e.shape, e.dtype),
        ],
        scratch_shapes=[
            pltpu.VMEM((modes, freqs, samples, 2, base), v.dtype),
            pltpu.VMEM((2, 2 * samples, kmax), F32),
            pltpu.SemaphoreType.DMA((modes, freqs)),
            pltpu.SemaphoreType.DMA((modes, freqs)),
        ],
        name="project",
        compiler_params=limit(MIB * 16),
        cost_estimate=cost(8 * modes * samples * freqs * base * kmax, v, e),
    )(pltpu.with_memory_space_constraint(v, pltpu.HBM), pltpu.with_memory_space_constraint(e, pltpu.HBM))


def rest_kernel(part_ref, v_ref, e_ref, give_ref, keep_ref):
    modes, freqs = e_ref.shape[:2]
    half, samples, _, base = v_ref.shape
    for j in range(half):
        x = v_ref[j].reshape(2 * samples, base)
        by_re = part_ref[j, 0] + jnp.dot(x, e_ref[half + j, freqs - 1, 0], preferred_element_type=F32)
        by_im = part_ref[j, 1] + jnp.dot(x, e_ref[half + j, freqs - 1, 1], preferred_element_type=F32)
        finish(j, by_re, by_im, give_ref, keep_ref)


def rest(part, v, e):
    half, samples, _, base = v.shape
    kmax = e.shape[-1]
    return pl.pallas_call(
        rest_kernel,
        in_specs=[VMEM] * 3,
        out_specs=[VMEM] * 2,
        out_shape=[
            jax.ShapeDtypeStruct((half, 2 * samples, kmax), BF16),
            jax.ShapeDtypeStruct((half, 2 * samples, kmax), F32),
        ],
        name="rest",
        compiler_params=limit(MIB * 4),
        cost_estimate=cost(8 * half * samples * base * kmax, v),
    )(part, v, e)


def power_kernel(keep_ref, a_ref, a_their_ref, b_ref, b_their_ref, total_ref, stats_ref):
    half, _, kmax = a_ref.shape
    stats = jnp.zeros((2, kmax), F32)
    for m in range(2 * half):
        mine, theirs = (a_ref, a_their_ref) if m < half else (b_ref, b_their_ref)
        total = mine[m % half].astype(F32) + theirs[m % half].astype(F32)
        total_ref[m] = total
        keep = keep_ref[m : m + 1]
        power = keep * jnp.sum(total * total, axis=0, keepdims=True)
        stats += jnp.where(side() == 1, jnp.concatenate([power, keep], axis=0), 0.0)
    stats_ref[...] = jnp.broadcast_to(stats[None], stats_ref.shape)


def power_of(keep, pairs, peers):
    half, rows, kmax = pairs[0].shape
    return pl.pallas_call(
        power_kernel,
        in_specs=[VMEM] * 5,
        out_specs=[VMEM] * 2,
        out_shape=[
            jax.ShapeDtypeStruct((2 * half, rows, kmax), F32),
            jax.ShapeDtypeStruct((peers, 2, kmax), F32),
        ],
        name="power",
        compiler_params=limit(MIB * 4),
    )(keep, *pairs)


def back_kernel(
    freq_size, keep_ref, stats_ref, mine_ref, other_ref, e_ref, coef_hbm, out_hbm, pair, flat, coef_buf, out_buf, coef_sem, out_sem
):
    modes, freqs, samples, _, base = out_buf.shape
    kmax = mine_ref.shape[-1]
    lanes = flat.shape[2]
    stats = jnp.sum(stats_ref[...], axis=0)
    power, count = stats[0:1] * F32(2 / freq_size), F32(samples) * (stats[1:2] * F32(2 / freq_size))
    scale = 1.0 / jnp.sqrt(power / jnp.maximum(count, 1.0) + 1e-06)
    contract = (((1,), (1,)), ((), ()))
    pending = []

    def send(src, dst, sem):
        copy = pltpu.make_async_copy(src, dst, sem)
        copy.start()
        pending.append(copy)

    for m in range(modes):
        gain = keep_ref[m : m + 1] * scale
        coef = jnp.where(side() == 1, mine_ref[m], other_ref[m]) * gain
        pair[:, :kmax] = coef.astype(BF16)
        pair[:, kmax:] = times_i(coef).astype(BF16)
        for i in range(kmax // lanes):
            flat[i] = coef[:, i * lanes : (i + 1) * lanes]
        for f in range(freqs):
            out = lax.dot_general(pair[:, :kmax], e_ref[m, f, 0], contract, preferred_element_type=F32)
            out += lax.dot_general(pair[:, kmax:], e_ref[m, f, 1], contract, preferred_element_type=F32)
            out_buf[m, f] = out.astype(BF16).reshape(samples, 2, base)
            if f == 0:
                for i in range(kmax // lanes):
                    for part in range(2):
                        every = flat[i, pl.ds(part, samples, stride=2), :]
                        coef_buf[m, part, :, i * lanes : (i + 1) * lanes] = every.astype(BF16)
                send(coef_buf.at[m], coef_hbm.at[m], coef_sem.at[m])
            send(out_buf.at[m, f], out_hbm.at[m, :, f], out_sem.at[m, f])
    for copy in pending:
        copy.wait()


def back(keep, freq_size, stats, mine, other, e):
    modes, freqs, _, base, kmax = e.shape
    samples = mine.shape[1] // 2
    return pl.pallas_call(
        functools.partial(back_kernel, freq_size),
        in_specs=[VMEM] * 5,
        out_specs=[HBM, HBM],
        out_shape=[
            jax.ShapeDtypeStruct((modes, 2, samples, kmax), BF16),
            jax.ShapeDtypeStruct((modes, samples, freqs, 2, base), BF16),
        ],
        scratch_shapes=[
            pltpu.VMEM((2 * samples, 2 * kmax), BF16),
            pltpu.VMEM((kmax // 128, 2 * samples, 128), F32),
            pltpu.VMEM((modes, 2, samples, kmax), BF16),
            pltpu.VMEM((modes, freqs, samples, 2, base), BF16),
            pltpu.SemaphoreType.DMA((modes,)),
            pltpu.SemaphoreType.DMA((modes, freqs)),
        ],
        name="back",
        compiler_params=limit(MIB * 16),
    )(keep, stats, mine, other, e)


def per_device(visibilities, eigenmodes, retained):
    freq_size, ma_size = lax.axis_size("freq"), lax.axis_size("ma")
    ranks = jnp.arange(eigenmodes.shape[-1], dtype=jnp.int32)
    keep = (ranks[None, :] < retained[:, None]).astype(F32)

    summing = range(1, freq_size, 2)

    def collect(x):
        return lax.ppermute(x, "freq", [(i - 1, i) for i in summing])

    def hand_back(x):
        return lax.ppermute(x, "freq", [(i, i - 1) for i in summing])

    def swap(x, bit):
        return lax.ppermute(x, "freq", [(i, i ^ bit) for i in summing])

    give_a, keep_a, part, v_last, e_vmem = project(visibilities, eigenmodes)
    give_b, keep_b = rest(part, v_last, e_vmem)
    pairs = []
    for give, kept in ((give_a, keep_a), (give_b, keep_b)):
        total = (kept + collect(give).astype(F32)).astype(BF16)
        bit = 2
        while 2 * bit < freq_size:
            total = (total.astype(F32) + swap(total, bit).astype(F32)).astype(BF16)
            bit *= 2
        pairs += [total, swap(total, bit)]
    mine, stats = power_of(keep, pairs, ma_size * freq_size)
    other = hand_back(mine)
    stats = lax.all_to_all(stats, ("ma", "freq"), 0, 0, tiled=True)
    return tuple(back(keep, freq_size, stats, mine, other, e_vmem))


def solution(mesh):
    return jax.shard_map(
        per_device,
        mesh=mesh,
        in_specs=(P("ma", None, "freq", None, None), P("ma", "freq", None, None, None), P("ma")),
        out_specs=(P("ma", None, None, None), P("ma", None, "freq", None, None)),
        check_vma=False,
    )
```

```python
import functools

import jax
import jax.numpy as jnp
from jax import lax
from jax.experimental import pallas as pl
from jax.experimental.pallas import tpu as pltpu
from jax.sharding import PartitionSpec as P


F32 = jnp.float32
BF16 = jnp.bfloat16
VMEM = pl.BlockSpec(memory_space=pltpu.VMEM)
HBM = pl.BlockSpec(memory_space=pltpu.HBM)
MIB = 1 << 20


def limit(vmem):
    return pltpu.CompilerParams(vmem_limit_bytes=vmem)


def cost(flops, *arrays):
    moved = sum(a.size * a.dtype.itemsize for a in arrays)
    return pl.CostEstimate(flops=flops, bytes_accessed=moved, transcendentals=0)


def side(bit=0):
    return ((lax.axis_index("freq") >> bit) & 1).astype(jnp.int32)


def times_i(x):
    up = pltpu.roll(x, x.shape[0] - 1, 0)
    down = pltpu.roll(x, 1, 0)
    even = (lax.broadcasted_iota(jnp.int32, x.shape, 0) & 1) == 0
    return jnp.where(even, -up, down)


def finish(j, by_re, by_im, give_ref, keep_ref):
    out = by_re - times_i(by_im)
    half = out.shape[0] // 2
    low, high = out[:half], out[half:]
    give_ref[j] = jnp.where(side() == 0, high, low).astype(give_ref.dtype)
    keep_ref[j] = jnp.where(side() == 0, low, high).astype(keep_ref.dtype)


def project_kernel(v_hbm, e_hbm, give_ref, keep_ref, part_ref, v_last, e_ref, v_buf, acc, v_sem, e_sem):
    modes, freqs = v_sem.shape
    samples, _, base = v_buf.shape[2:]
    half = modes // 2
    copies = []
    for m in range(modes):
        for f in range(freqs):
            late = m >= half and f == freqs - 1
            v_to = v_last.at[m - half] if late else v_buf.at[m, f]
            e_copy = pltpu.make_async_copy(e_hbm.at[m, f], e_ref.at[m, f], e_sem.at[m, f])
            v_copy = pltpu.make_async_copy(v_hbm.at[m, :, f], v_to, v_sem.at[m, f])
            e_copy.start()
            v_copy.start()
            copies.append((e_copy, v_copy))
    for m in range(modes):
        for f in range(freqs):
            for copy in copies[m * freqs + f]:
                copy.wait()
            if m >= half and f == freqs - 1:
                continue
            x = v_buf[m, f].reshape(2 * samples, base)
            by_re = jnp.dot(x, e_ref[m, f, 0], preferred_element_type=F32)
            by_im = jnp.dot(x, e_ref[m, f, 1], preferred_element_type=F32)
            sums = part_ref.at[m - half] if m >= half else acc
            if f > 0:
                by_re += sums[0]
                by_im += sums[1]
            if m >= half or f < freqs - 1:
                sums[0] = by_re
                sums[1] = by_im
            else:
                finish(m, by_re, by_im, give_ref, keep_ref)


def project(v, e):
    modes, samples, freqs, _, base = v.shape
    kmax = e.shape[-1]
    half = modes // 2
    return pl.pallas_call(
        project_kernel,
        in_specs=[HBM, HBM],
        out_specs=[VMEM] * 5,
        out_shape=[
            jax.ShapeDtypeStruct((half, samples, kmax), BF16),
            jax.ShapeDtypeStruct((half, samples, kmax), F32),
            jax.ShapeDtypeStruct((half, 2, 2 * samples, kmax), F32),
            jax.ShapeDtypeStruct((half, samples, 2, base), v.dtype),
            jax.ShapeDtypeStruct(e.shape, e.dtype),
        ],
        scratch_shapes=[
            pltpu.VMEM((modes, freqs, samples, 2, base), v.dtype),
            pltpu.VMEM((2, 2 * samples, kmax), F32),
            pltpu.SemaphoreType.DMA((modes, freqs)),
            pltpu.SemaphoreType.DMA((modes, freqs)),
        ],
        name="project",
        compiler_params=limit(MIB * 16),
        cost_estimate=cost(8 * modes * samples * freqs * base * kmax, v, e),
    )(pltpu.with_memory_space_constraint(v, pltpu.HBM), pltpu.with_memory_space_constraint(e, pltpu.HBM))


def rest_kernel(part_ref, v_ref, e_ref, give_ref, keep_ref):
    _, freqs = e_ref.shape[:2]
    half, samples, _, base = v_ref.shape
    for j in range(half):
        x = v_ref[j].reshape(2 * samples, base)
        by_re = part_ref[j, 0] + jnp.dot(x, e_ref[half + j, freqs - 1, 0], preferred_element_type=F32)
        by_im = part_ref[j, 1] + jnp.dot(x, e_ref[half + j, freqs - 1, 1], preferred_element_type=F32)
        finish(j, by_re, by_im, give_ref, keep_ref)


def rest(part, v, e):
    half, samples, _, base = v.shape
    kmax = e.shape[-1]
    return pl.pallas_call(
        rest_kernel,
        in_specs=[VMEM] * 3,
        out_specs=[VMEM] * 2,
        out_shape=[
            jax.ShapeDtypeStruct((half, samples, kmax), BF16),
            jax.ShapeDtypeStruct((half, samples, kmax), F32),
        ],
        name="rest",
        compiler_params=limit(MIB * 4),
        cost_estimate=cost(8 * half * samples * base * kmax, v),
    )(part, v, e)


def split_kernel(mine_ref, theirs_ref, give_ref, keep_ref):
    half, rows, _ = give_ref.shape
    for j in range(half):
        total = mine_ref[j] + theirs_ref[j].astype(F32)
        low, high = total[:rows], total[rows:]
        give_ref[j] = jnp.where(side(1) == 0, high, low).astype(give_ref.dtype)
        keep_ref[j] = jnp.where(side(1) == 0, low, high)


def split(mine, theirs):
    half, rows, kmax = mine.shape
    return pl.pallas_call(
        split_kernel,
        in_specs=[VMEM] * 2,
        out_specs=[VMEM] * 2,
        out_shape=[
            jax.ShapeDtypeStruct((half, rows // 2, kmax), BF16),
            jax.ShapeDtypeStruct((half, rows // 2, kmax), F32),
        ],
        name="split",
        compiler_params=limit(MIB * 2),
    )(mine, theirs)


def power_kernel(freq_size, keep_ref, quarter_ref, b_ref, b_their_ref, total_ref, stats_ref):
    half, _, kmax = b_ref.shape
    stats = jnp.zeros((2, kmax), F32)
    for m in range(2 * half):
        if m < half:
            total, copies = quarter_ref[m].astype(F32), freq_size // 4
        else:
            total, copies = b_ref[m - half].astype(F32) + b_their_ref[m - half].astype(F32), freq_size // 2
            total_ref[m - half] = total
        keep = keep_ref[m : m + 1]
        power = keep * jnp.sum(total * total, axis=0, keepdims=True) * F32(1.0 / copies)
        stats += jnp.concatenate([power, keep * F32(1.0 / freq_size)], axis=0)
    stats_ref[...] = jnp.broadcast_to(stats[None], stats_ref.shape)


def power_of(keep, freq_size, quarter, mine, theirs, peers):
    kmax = mine.shape[-1]
    return pl.pallas_call(
        functools.partial(power_kernel, freq_size),
        in_specs=[VMEM] * 4,
        out_specs=[VMEM] * 2,
        out_shape=[
            jax.ShapeDtypeStruct(mine.shape, F32),
            jax.ShapeDtypeStruct((peers, 2, kmax), F32),
        ],
        name="power",
        compiler_params=limit(MIB * 4),
    )(keep, quarter, mine, theirs)


def pool_kernel(samples, stats_ref, scale_ref):
    stats = jnp.sum(stats_ref[...], axis=0)
    power, count = stats[0:1], F32(samples) * stats[1:2]
    scale_ref[...] = 1.0 / jnp.sqrt(power / jnp.maximum(count, 1.0) + 1e-06)


def pool(stats, samples):
    return pl.pallas_call(
        functools.partial(pool_kernel, samples),
        in_specs=[VMEM],
        out_specs=VMEM,
        out_shape=jax.ShapeDtypeStruct((1, stats.shape[-1]), F32),
        name="pool",
        compiler_params=limit(MIB),
    )(stats)


def half_pieces(j, mine_ref, other_ref):
    for c in range(2):
        yield c * mine_ref.shape[1], jnp.where(side() == c, mine_ref[j], other_ref[j])


def quarter_pieces(j, own_ref, chip_ref, core_ref):
    own, chip, core, both = [q.astype(F32) for q in (own_ref[j], chip_ref[j], core_ref[0, j], core_ref[1, j])]
    for c in range(2):
        near, far = jnp.where(side() == c, own, core), jnp.where(side() == c, chip, both)
        for y in range(2):
            yield (2 * c + y) * own.shape[0], jnp.where(side(1) == y, near, far)


def filter_mode(m, pieces, keep_ref, scale_ref, e_ref, pair, flat, coef_ref, out_ref, after_coef, after_out):
    freqs, samples, _, base = out_ref.shape
    kmax = pair.shape[1] // 2
    lanes = flat.shape[2]
    contract = (((1,), (1,)), ((), ()))
    gain = keep_ref[m : m + 1] * scale_ref[...]
    for start, proj in pieces:
        coef = proj * gain
        at = slice(start, start + coef.shape[0])
        pair[at, :kmax] = coef.astype(BF16)
        pair[at, kmax:] = times_i(coef).astype(BF16)
        for i in range(kmax // lanes):
            flat[i, at, :] = coef[:, i * lanes : (i + 1) * lanes]
    for f in range(freqs):
        out = lax.dot_general(pair[:, :kmax], e_ref[m, f, 0], contract, preferred_element_type=F32)
        out += lax.dot_general(pair[:, kmax:], e_ref[m, f, 1], contract, preferred_element_type=F32)
        out_ref[f] = out.astype(BF16).reshape(samples, 2, base)
        if f == 0:
            for i in range(kmax // lanes):
                for part in range(2):
                    every = flat[i, pl.ds(part, samples, stride=2), :]
                    coef_ref[part, :, i * lanes : (i + 1) * lanes] = every.astype(BF16)
            after_coef()
        after_out(f)


def nothing(*_):
    pass


def back_b_kernel(keep_ref, scale_ref, mine_ref, other_ref, e_ref, coef_ref, out_ref, pair, flat):
    half = mine_ref.shape[0]
    for j in range(half):
        rows = half_pieces(j, mine_ref, other_ref)
        filter_mode(half + j, rows, keep_ref, scale_ref, e_ref, pair, flat, coef_ref.at[j], out_ref.at[j], nothing, nothing)


def back_a_kernel(
    keep_ref, scale_ref, own_ref, chip_ref, core_ref, coef_b, out_b, e_ref, coef_hbm, out_hbm, pair, flat, coef_buf, out_buf, coef_sem, out_sem
):
    half, freqs = out_buf.shape[:2]
    pending = []

    def send(src, dst, sem):
        copy = pltpu.make_async_copy(src, dst, sem)
        copy.start()
        pending.append(copy)

    for j in range(half):
        send(coef_b.at[j], coef_hbm.at[half + j], coef_sem.at[half + j])
        for f in range(freqs):
            send(out_b.at[j, f], out_hbm.at[half + j, :, f], out_sem.at[half + j, f])
    for j in range(half):
        filter_mode(
            j, quarter_pieces(j, own_ref, chip_ref, core_ref), keep_ref, scale_ref, e_ref, pair, flat, coef_buf.at[j], out_buf.at[j],
            lambda j=j: send(coef_buf.at[j], coef_hbm.at[j], coef_sem.at[j]),
            lambda f, j=j: send(out_buf.at[j, f], out_hbm.at[j, :, f], out_sem.at[j, f]),
        )
    for copy in pending:
        copy.wait()


def back_b(keep, scale, mine, other, e):
    _, freqs, _, base, kmax = e.shape
    half, samples = mine.shape[:2]
    return pl.pallas_call(
        back_b_kernel,
        in_specs=[VMEM] * 5,
        out_specs=[VMEM] * 2,
        out_shape=[
            jax.ShapeDtypeStruct((half, 2, samples, kmax), BF16),
            jax.ShapeDtypeStruct((half, freqs, samples, 2, base), BF16),
        ],
        scratch_shapes=[pltpu.VMEM((2 * samples, 2 * kmax), BF16), pltpu.VMEM((kmax // 128, 2 * samples, 128), F32)],
        name="back_b",
        compiler_params=limit(MIB * 16),
        cost_estimate=cost(8 * half * samples * freqs * base * kmax, mine, other),
    )(keep, scale, mine, other, e)


def back_a(keep, scale, quarters, done, e):
    modes, freqs, _, base, kmax = e.shape
    half, _, samples, _ = done[0].shape
    return pl.pallas_call(
        back_a_kernel,
        in_specs=[VMEM] * 8,
        out_specs=[HBM, HBM],
        out_shape=[
            jax.ShapeDtypeStruct((modes, 2, samples, kmax), BF16),
            jax.ShapeDtypeStruct((modes, samples, freqs, 2, base), BF16),
        ],
        scratch_shapes=[
            pltpu.VMEM((2 * samples, 2 * kmax), BF16),
            pltpu.VMEM((kmax // 128, 2 * samples, 128), F32),
            pltpu.VMEM((half, 2, samples, kmax), BF16),
            pltpu.VMEM((half, freqs, samples, 2, base), BF16),
            pltpu.SemaphoreType.DMA((modes,)),
            pltpu.SemaphoreType.DMA((modes, freqs)),
        ],
        name="back_a",
        compiler_params=limit(MIB * 16),
    )(keep, scale, *quarters, *done, e)


def filter_modes(visibilities, eigenmodes, retained):
    freq_size, ma_size = lax.axis_size("freq"), lax.axis_size("ma")
    ranks = jnp.arange(eigenmodes.shape[-1], dtype=jnp.int32)
    keep = (ranks[None, :] < retained[:, None]).astype(F32)

    def swap(x, bit):
        return lax.ppermute(x, "freq", [(i, i ^ bit) for i in range(freq_size)])

    def over_chips(total):
        bit = 2
        while 2 * bit < freq_size:
            total = (total.astype(F32) + swap(total, bit).astype(F32)).astype(BF16)
            bit *= 2
        return total, swap(total, bit)

    give_a, keep_a, part, v_last, e_vmem = project(visibilities, eigenmodes)
    give_b, keep_b = rest(part, v_last, e_vmem)
    give_a, keep_a = split(keep_a, swap(give_a, 1))
    quarter = keep_a + swap(give_a, 2).astype(F32)
    bit = 4
    while bit < freq_size:
        quarter = quarter + swap(quarter.astype(BF16), bit).astype(F32)
        bit *= 2
    quarter = quarter.astype(BF16)
    total, theirs = over_chips((keep_b + swap(give_b, 1).astype(F32)).astype(BF16))
    chip = swap(quarter, 2)
    mine, stats = power_of(keep, freq_size, quarter, total, theirs, ma_size * freq_size)
    other = swap(mine, 1)
    stats = lax.all_to_all(stats, ("ma", "freq"), 0, 0, tiled=True)
    scale = pool(stats, visibilities.shape[1])
    core = swap(jnp.stack([quarter, chip]), 1)
    done = back_b(keep, scale, mine, other, e_vmem)
    return tuple(back_a(keep, scale, (quarter, chip, core), done, e_vmem))


def solution(mesh):
    return jax.shard_map(
        filter_modes,
        mesh=mesh,
        in_specs=(P("ma", None, "freq", None, None), P("ma", "freq", None, None, None), P("ma")),
        out_specs=(P("ma", None, None, None), P("ma", None, "freq", None, None)),
        check_vma=False,
    )
```

```python
import functools

import jax
import jax.numpy as jnp
from jax import lax
from jax.experimental import pallas as pl
from jax.experimental.pallas import tpu as pltpu
from jax.sharding import PartitionSpec as P


F32 = jnp.float32
BF16 = jnp.bfloat16
VMEM = pl.BlockSpec(memory_space=pltpu.VMEM)
HBM = pl.BlockSpec(memory_space=pltpu.HBM)
MIB = 1 << 20


def limit(vmem):
    return pltpu.CompilerParams(vmem_limit_bytes=vmem)


def cost(flops, *arrays):
    moved = sum(a.size * a.dtype.itemsize for a in arrays)
    return pl.CostEstimate(flops=flops, bytes_accessed=moved, transcendentals=0)


def side(bit=0):
    return ((lax.axis_index("freq") >> bit) & 1).astype(jnp.int32)


def times_i(x):
    up = pltpu.roll(x, x.shape[0] - 1, 0)
    down = pltpu.roll(x, 1, 0)
    even = (lax.broadcasted_iota(jnp.int32, x.shape, 0) & 1) == 0
    return jnp.where(even, -up, down)


def finish(j, by_re, by_im, give_ref, keep_ref):
    out = by_re - times_i(by_im)
    half = out.shape[0] // 2
    low, high = out[:half], out[half:]
    give_ref[j] = jnp.where(side() == 0, high, low).astype(give_ref.dtype)
    keep_ref[j] = jnp.where(side() == 0, low, high).astype(keep_ref.dtype)


def project_kernel(v_hbm, e_hbm, give_ref, keep_ref, part_ref, v_last, e_ref, v_buf, acc, v_sem, e_sem):
    modes, freqs = v_sem.shape
    samples, _, base = v_buf.shape[2:]
    half = modes // 2
    copies = []
    for m in range(modes):
        for f in range(freqs):
            late = m >= half and f == freqs - 1
            v_to = v_last.at[m - half] if late else v_buf.at[m, f]
            e_copy = pltpu.make_async_copy(e_hbm.at[m, f], e_ref.at[m, f], e_sem.at[m, f])
            v_copy = pltpu.make_async_copy(v_hbm.at[m, :, f], v_to, v_sem.at[m, f])
            e_copy.start()
            v_copy.start()
            copies.append((e_copy, v_copy))
    for m in range(modes):
        for f in range(freqs):
            for copy in copies[m * freqs + f]:
                copy.wait()
            if m >= half and f == freqs - 1:
                continue
            x = v_buf[m, f].reshape(2 * samples, base)
            by_re = jnp.dot(x, e_ref[m, f, 0], preferred_element_type=F32)
            by_im = jnp.dot(x, e_ref[m, f, 1], preferred_element_type=F32)
            sums = part_ref.at[m - half] if m >= half else acc
            if f > 0:
                by_re += sums[0]
                by_im += sums[1]
            if m >= half or f < freqs - 1:
                sums[0] = by_re
                sums[1] = by_im
            else:
                finish(m, by_re, by_im, give_ref, keep_ref)


def project(v, e):
    modes, samples, freqs, _, base = v.shape
    kmax = e.shape[-1]
    half = modes // 2
    return pl.pallas_call(
        project_kernel,
        in_specs=[HBM, HBM],
        out_specs=[VMEM] * 5,
        out_shape=[
            jax.ShapeDtypeStruct((half, samples, kmax), BF16),
            jax.ShapeDtypeStruct((half, samples, kmax), F32),
            jax.ShapeDtypeStruct((half, 2, 2 * samples, kmax), F32),
            jax.ShapeDtypeStruct((half, samples, 2, base), v.dtype),
            jax.ShapeDtypeStruct(e.shape, e.dtype),
        ],
        scratch_shapes=[
            pltpu.VMEM((modes, freqs, samples, 2, base), v.dtype),
            pltpu.VMEM((2, 2 * samples, kmax), F32),
            pltpu.SemaphoreType.DMA((modes, freqs)),
            pltpu.SemaphoreType.DMA((modes, freqs)),
        ],
        name="project",
        compiler_params=limit(MIB * 16),
        cost_estimate=cost(8 * modes * samples * freqs * base * kmax, v, e),
    )(pltpu.with_memory_space_constraint(v, pltpu.HBM), pltpu.with_memory_space_constraint(e, pltpu.HBM))


def rest_kernel(part_ref, v_ref, e_ref, give_ref, keep_ref):
    _, freqs = e_ref.shape[:2]
    half, samples, _, base = v_ref.shape
    for j in range(half):
        x = v_ref[j].reshape(2 * samples, base)
        by_re = part_ref[j, 0] + jnp.dot(x, e_ref[half + j, freqs - 1, 0], preferred_element_type=F32)
        by_im = part_ref[j, 1] + jnp.dot(x, e_ref[half + j, freqs - 1, 1], preferred_element_type=F32)
        finish(j, by_re, by_im, give_ref, keep_ref)


def rest(part, v, e):
    half, samples, _, base = v.shape
    kmax = e.shape[-1]
    return pl.pallas_call(
        rest_kernel,
        in_specs=[VMEM] * 3,
        out_specs=[VMEM] * 2,
        out_shape=[
            jax.ShapeDtypeStruct((half, samples, kmax), BF16),
            jax.ShapeDtypeStruct((half, samples, kmax), F32),
        ],
        name="rest",
        compiler_params=limit(MIB * 4),
        cost_estimate=cost(8 * half * samples * base * kmax, v),
    )(part, v, e)


def split_kernel(mine_ref, theirs_ref, give_ref, keep_ref):
    half, rows, _ = give_ref.shape
    for j in range(half):
        total = mine_ref[j] + theirs_ref[j].astype(F32)
        low, high = total[:rows], total[rows:]
        give_ref[j] = jnp.where(side(1) == 0, high, low).astype(give_ref.dtype)
        keep_ref[j] = jnp.where(side(1) == 0, low, high)


def split(mine, theirs):
    half, rows, kmax = mine.shape
    return pl.pallas_call(
        split_kernel,
        in_specs=[VMEM] * 2,
        out_specs=[VMEM] * 2,
        out_shape=[
            jax.ShapeDtypeStruct((half, rows // 2, kmax), BF16),
            jax.ShapeDtypeStruct((half, rows // 2, kmax), F32),
        ],
        name="split",
        compiler_params=limit(MIB * 2),
    )(mine, theirs)


def power_kernel(freq_size, keep_ref, quarter_ref, b_ref, b_their_ref, total_ref, stats_ref):
    half, _, kmax = b_ref.shape
    stats = jnp.zeros((2, kmax), F32)
    for m in range(2 * half):
        if m < half:
            total, copies = quarter_ref[m].astype(F32), freq_size // 4
            total_ref[m, b_ref.shape[1] :] = total
        else:
            total, copies = b_ref[m - half].astype(F32) + b_their_ref[m - half].astype(F32), freq_size // 2
            total_ref[m - half, : b_ref.shape[1]] = total
        keep = keep_ref[m : m + 1]
        power = keep * jnp.sum(total * total, axis=0, keepdims=True) * F32(1.0 / copies)
        stats += jnp.concatenate([power, keep * F32(1.0 / freq_size)], axis=0)
    stats_ref[...] = jnp.broadcast_to(stats[None], stats_ref.shape)


def power_of(keep, freq_size, quarter, mine, theirs, peers):
    kmax = mine.shape[-1]
    return pl.pallas_call(
        functools.partial(power_kernel, freq_size),
        in_specs=[VMEM] * 4,
        out_specs=[VMEM] * 2,
        out_shape=[
            jax.ShapeDtypeStruct((mine.shape[0], mine.shape[1] + quarter.shape[1], kmax), F32),
            jax.ShapeDtypeStruct((peers, 2, kmax), F32),
        ],
        name="power",
        compiler_params=limit(MIB * 4),
    )(keep, quarter, mine, theirs)


def pool_kernel(samples, stats_ref, scale_ref):
    stats = jnp.sum(stats_ref[...], axis=0)
    power, count = stats[0:1], F32(samples) * stats[1:2]
    scale_ref[...] = 1.0 / jnp.sqrt(power / jnp.maximum(count, 1.0) + 1e-06)


def pool(stats, samples):
    return pl.pallas_call(
        functools.partial(pool_kernel, samples),
        in_specs=[VMEM],
        out_specs=VMEM,
        out_shape=jax.ShapeDtypeStruct((1, stats.shape[-1]), F32),
        name="pool",
        compiler_params=limit(MIB),
    )(stats)


def pieces(m, c, y, quarters, mine_ref, other_ref):
    half = mine_ref.shape[0]
    if m < half:
        own, chip, both = [q[m].astype(F32) for q in quarters]
        rows = own.shape[0]
        core = other_ref[m, 2 * rows :]
        for c_of in range(2):
            near, far = jnp.where(c == c_of, own, core), jnp.where(c == c_of, chip, both)
            for y_of in range(2):
                yield (2 * c_of + y_of) * rows, jnp.where(y == y_of, near, far)
    else:
        rows = 2 * quarters[0].shape[1]
        mine, other = mine_ref[m - half, :rows], other_ref[m - half, :rows]
        for c_of in range(2):
            yield c_of * mine.shape[0], jnp.where(c == c_of, mine, other)


def back_kernel(
    keep_ref, scale_ref, q0_ref, q2_ref, q3_ref, mine_ref, other_ref, e_ref, coef_hbm, out_hbm, pair, flat, coef_buf, out_buf, coef_sem, out_sem
):
    modes, freqs, samples, _, base = out_buf.shape
    kmax = mine_ref.shape[-1]
    lanes = flat.shape[2]
    contract = (((1,), (1,)), ((), ()))
    pending = []

    def send(src, dst, sem):
        copy = pltpu.make_async_copy(src, dst, sem)
        copy.start()
        pending.append(copy)

    for m in range(modes):
        gain = keep_ref[m : m + 1] * scale_ref[...]
        for start, proj in pieces(m, side(), side(1), (q0_ref, q2_ref, q3_ref), mine_ref, other_ref):
            coef = proj * gain
            at = slice(start, start + coef.shape[0])
            pair[at, :kmax] = coef.astype(BF16)
            pair[at, kmax:] = times_i(coef).astype(BF16)
            for i in range(kmax // lanes):
                flat[i, at, :] = coef[:, i * lanes : (i + 1) * lanes]
        for f in range(freqs):
            out = lax.dot_general(pair[:, :kmax], e_ref[m, f, 0], contract, preferred_element_type=F32)
            out += lax.dot_general(pair[:, kmax:], e_ref[m, f, 1], contract, preferred_element_type=F32)
            out_buf[m, f] = out.astype(BF16).reshape(samples, 2, base)
            if f == 0:
                for i in range(kmax // lanes):
                    for part in range(2):
                        every = flat[i, pl.ds(part, samples, stride=2), :]
                        coef_buf[m, part, :, i * lanes : (i + 1) * lanes] = every.astype(BF16)
                send(coef_buf.at[m], coef_hbm.at[m], coef_sem.at[m])
            send(out_buf.at[m, f], out_hbm.at[m, :, f], out_sem.at[m, f])
    for copy in pending:
        copy.wait()


def back(keep, scale, quarters, mine, other, e):
    modes, freqs, _, base, kmax = e.shape
    samples = 2 * quarters[0].shape[1]
    return pl.pallas_call(
        back_kernel,
        in_specs=[VMEM] * 8,
        out_specs=[HBM, HBM],
        out_shape=[
            jax.ShapeDtypeStruct((modes, 2, samples, kmax), BF16),
            jax.ShapeDtypeStruct((modes, samples, freqs, 2, base), BF16),
        ],
        scratch_shapes=[
            pltpu.VMEM((2 * samples, 2 * kmax), BF16),
            pltpu.VMEM((kmax // 128, 2 * samples, 128), F32),
            pltpu.VMEM((modes, 2, samples, kmax), BF16),
            pltpu.VMEM((modes, freqs, samples, 2, base), BF16),
            pltpu.SemaphoreType.DMA((modes,)),
            pltpu.SemaphoreType.DMA((modes, freqs)),
        ],
        name="back",
        compiler_params=limit(MIB * 16),
    )(keep, scale, *quarters, mine, other, e)


def filter_modes(visibilities, eigenmodes, retained):
    freq_size, ma_size = lax.axis_size("freq"), lax.axis_size("ma")
    ranks = jnp.arange(eigenmodes.shape[-1], dtype=jnp.int32)
    keep = (ranks[None, :] < retained[:, None]).astype(F32)

    def swap(x, bit):
        return lax.ppermute(x, "freq", [(i, i ^ bit) for i in range(freq_size)])

    def over_chips(total):
        bit = 2
        while 2 * bit < freq_size:
            total = (total.astype(F32) + swap(total, bit).astype(F32)).astype(BF16)
            bit *= 2
        return total, swap(total, bit)

    give_a, keep_a, part, v_last, e_vmem = project(visibilities, eigenmodes)
    give_b, keep_b = rest(part, v_last, e_vmem)
    give_a, keep_a = split(keep_a, swap(give_a, 1))
    quarter = keep_a + swap(give_a, 2).astype(F32)
    bit = 4
    while bit < freq_size:
        quarter = quarter + swap(quarter.astype(BF16), bit).astype(F32)
        bit *= 2
    quarter = quarter.astype(BF16)
    total, theirs = over_chips((keep_b + swap(give_b, 1).astype(F32)).astype(BF16))
    quarters = [quarter]
    for bits in (2, 3):
        quarters.append(swap(quarter, bits))
    mine, stats = power_of(keep, freq_size, quarter, total, theirs, ma_size * freq_size)
    other = swap(mine, 1)
    scale = pool(lax.all_to_all(stats, ("ma", "freq"), 0, 0, tiled=True), visibilities.shape[1])
    return tuple(back(keep, scale, quarters, mine, other, e_vmem))


def solution(mesh):
    return jax.shard_map(
        filter_modes,
        mesh=mesh,
        in_specs=(P("ma", None, "freq", None, None), P("ma", "freq", None, None, None), P("ma")),
        out_specs=(P("ma", None, None, None), P("ma", None, "freq", None, None)),
        check_vma=False,
    )
```
